32 devices in a mesh: sub: 8 (over z, x), fdr: 4 (over y, core).
Axes of the slice: x: 2, y: 2, z: 4, core: 2. Of those that a mesh axis runs over, the one named last changes fastest.
Arguments:
- inverse: bfloat16 [1024, 256, 256], P(('sub', 'fdr')), may hold values from -1 to 1
- cost: float32 [1024, 256, 128], P(('sub', 'fdr')), may hold values from -6 to 6
- lower_limit: float32 [1024, 256], P(('sub', 'fdr')), may hold values from -1.5 to -0.5
- upper_limit: float32 [1024, 256], P(('sub', 'fdr')), may hold values from 0.5 to 1.5
- iface_rows: int32 [1024, 6], P(('sub', 'fdr')), may hold values from 0 to 255, as said below
- substation_of: int32 [1024], P(('sub', 'fdr')), may hold values from 0 to 255, as said below
- live_count: int32 [32], P(('sub', 'fdr')), may hold values from 16 to 32
- reserve_weight: float32 [256], P('sub'), may hold values from 0.5 to 4
- reserve_target: float32 [256, 6, 128], P('sub'), may hold values from -6 to 6
Outputs:
- duals: float32 [1024, 6, 128], P(('sub', 'fdr'))
- consensus: float32 [256, 6, 128], P('sub')
- residual_norms: float32 [5, 2], replicated
- setpoints: float32 [1024, 256, 128], P(('sub', 'fdr'))
The draws below stay inside these ranges and needn't reach their ends.
Inputs may be any that keep to these rules, and one draw needn't show every extreme that they name: `iface_rows`: each feeder's 6 interface rows are distinct. `substation_of`: of one device's 32 slots at most 6 hang from substations of one owner block (substations k * 32 to k * 32 + 31); for each index of fdr some block gets exactly 6 slots from every device with that index. `live_count`: a device's live feeders fill its first slots; the other slots hold unused data.
All inputs are finite; a program needn't handle non-finite values.
Results may differ from the reference program's by a relative error of at most 0.0069.
Values sent between devices are 32-bit elements; how exact they have to be, the bound alone decides.
No kernel may reach another device: no remote copies, remote signals or barrier semaphores. Data moves between devices by JAX's collectives and lax.ppermute only.
A program may use at most 128 MiB of HBM per device.

```python
import math
import jax
import jax.numpy as jnp
from jax import lax

KKT = 256
IFC = 6
SC = 128
FDEV = 32
SDEV = 32
ITERS = 5
F = 1024
S = 256
CAP = 6
N_SUB = 8
N_FDR = 4
DEVICES = 32


def draw_inverse(key, part):
    key_a = jax.random.fold_in(key, 11)
    key_b = jax.random.fold_in(key, 12)
    noise_draw = jax.random.normal(key_a, (F, KKT, KKT), jnp.float32)
    symmetric = (noise_draw + jnp.swapaxes(noise_draw, 1, 2)) * (0.25 / KKT ** 0.5)
    diag_vals = jax.random.uniform(key_b, (F, KKT), jnp.float32, 0.3, 0.8)
    identity_matrix = jnp.eye(KKT, dtype=jnp.float32)
    matrix = symmetric + diag_vals[:, :, None] * identity_matrix[None, :, :]
    matrix = jnp.clip(matrix, -1.0, 1.0)
    return matrix.astype(jnp.bfloat16)


def draw_iface_rows(key, part):
    scores = jax.random.randint(jax.random.fold_in(key, 21), (F, KKT), 0, KKT)
    scores = scores * KKT + jnp.arange(KKT, dtype=jnp.int32)[None, :]
    ranking = jnp.argsort(scores, axis=1, stable=True)
    return ranking[:, :IFC].astype(jnp.int32)


def draw_substation_of(key, part):
    slot_total = N_SUB * CAP
    entry = jnp.arange(slot_total, dtype=jnp.int32)
    entry_group = entry // CAP
    column_first = jax.random.randint(jax.random.fold_in(key, 31), (N_FDR,), 0, N_SUB).astype(jnp.int32)
    device_first = jnp.tile(column_first, DEVICES // N_FDR)
    noise_int = jax.random.randint(jax.random.fold_in(key, 32), (DEVICES, slot_total), 0, 65536).astype(jnp.int32)
    priority = entry_group[None, :] == device_first[:, None]
    scores = jnp.where(priority, entry[None, :], (noise_int + 1) * slot_total + entry[None, :])
    ranking = jnp.argsort(scores, axis=1, stable=True)
    chosen = entry_group[ranking[:, :FDEV]]
    shuffle_scores = jax.random.randint(jax.random.fold_in(key, 33), (DEVICES, FDEV), 0, 65536).astype(jnp.int32) * FDEV + jnp.arange(FDEV, dtype=jnp.int32)[None, :]
    shuffle = jnp.argsort(shuffle_scores, axis=1, stable=True)
    groups = jnp.take_along_axis(chosen, shuffle, axis=1)
    within = jax.random.randint(jax.random.fold_in(key, 34), (DEVICES, FDEV), 0, SDEV).astype(jnp.int32)
    return (groups * SDEV + within).reshape(DEVICES * FDEV).astype(jnp.int32)


def set_ends(result, stream_key, low, top_value):
    extent = result.shape
    index_at = [jax.random.randint(jax.random.fold_in(stream_key, axis), (), 0, extent[axis]) for axis in range(len(extent))]
    result = result.at[tuple(index_at)].set(low)
    longest = extent.index(max(extent))
    index_at[longest] = (index_at[longest] + 1) % extent[longest]
    return result.at[tuple(index_at)].set(top_value)


def shard_levels(rng, extent, pieces, least, top_value):
    factor_of, own = 1.0, jax.random.fold_in(rng, 6)
    for position, blocks in pieces:
        draws = jnp.exp(jax.random.uniform(jax.random.fold_in(own, position), (blocks,), jnp.float32, least / len(pieces), top_value / len(pieces)))
        factor_of = factor_of * jnp.repeat(draws, extent[position] // blocks).reshape([-1 if axis == position else 1 for axis in range(len(extent))])
    return factor_of


def normal_values(stream_key, dims, width, limit, cuts=(), held_as=jnp.bfloat16):
    loudness = shard_levels(stream_key, dims, cuts, -0.22, 0.18) if cuts else 1.0
    array = jax.random.normal(stream_key, dims, jnp.float32) * width * loudness
    return jnp.minimum(jnp.maximum(array, -limit), limit).astype(held_as)


def setup_inputs(seed: int = 0) -> dict:
    streams_of = jax.random.split(jax.random.key(seed), 10)
    return {
        "inverse": draw_inverse(jax.random.fold_in(streams_of[9], 71), 0),
        "cost": normal_values(streams_of[1], (F, KKT, SC), 1.0, 6.0, ((0, 32),), jnp.float32),
        "lower_limit": jnp.clip(-1.5 + 1.0 * jax.random.uniform(streams_of[2], (F, KKT), jnp.float32) ** shard_levels(streams_of[2], (F, KKT), ((0, 32),), -0.2, 0.2), -1.5, -0.5),
        "upper_limit": jnp.clip(0.5 + 1.0 * jax.random.uniform(streams_of[3], (F, KKT), jnp.float32) ** shard_levels(streams_of[3], (F, KKT), ((0, 32),), -0.2, 0.2), 0.5, 1.5),
        "iface_rows": draw_iface_rows(jax.random.fold_in(streams_of[9], 71), 0),
        "substation_of": draw_substation_of(jax.random.fold_in(streams_of[9], 71), 0),
        "live_count": set_ends(jax.random.randint(streams_of[6], (DEVICES,), FDEV // 2, FDEV + 1), jax.random.fold_in(streams_of[6], 1), FDEV // 2, FDEV).astype(jnp.int32),
        "reserve_weight": jnp.clip(jnp.exp(math.log(4.0) - 2.0794415 * jax.random.uniform(streams_of[7], (S,), jnp.float32) ** shard_levels(streams_of[7], (S,), ((0, 8),), -0.2, 0.2)), 0.5, 4.0),
        "reserve_target": normal_values(streams_of[8], (S, IFC, SC), 1.0, 6.0, ((0, 8),), jnp.float32),
    }


penalty = 2.0

def solve_block(operands):
    block_inverse, block_rhs = operands
    return jnp.einsum('fkj,fjs->fks', block_inverse.astype(jnp.float32), block_rhs.astype(jnp.float32), precision=lax.Precision.HIGHEST)

def reference(inverse, cost, lower_limit, upper_limit, iface_rows, substation_of, live_count, reserve_weight, reserve_target):
    slot_total = inverse.shape[0]
    slot_number = jnp.arange(slot_total, dtype=jnp.int32) % FDEV
    active = (slot_number < jnp.repeat(live_count, FDEV)).astype(jnp.float32)
    members = jax.ops.segment_sum(active, substation_of, num_segments=S)
    feeder_index = jnp.arange(slot_total, dtype=jnp.int32)[:, None]
    blocks = inverse.reshape(slot_total // FDEV, FDEV, KKT, KKT)
    scaled_dual = jnp.zeros((slot_total, IFC, SC), jnp.float32)
    local_consensus = jnp.zeros((slot_total, IFC, SC), jnp.float32)
    anchor = jnp.zeros((slot_total, KKT, SC), jnp.float32)
    consensus = jnp.zeros((S, IFC, SC), jnp.float32)
    history = []
    for iteration in range(ITERS):
        right_side = (anchor - cost).at[feeder_index, iface_rows].add(penalty * (local_consensus - scaled_dual)).astype(jnp.bfloat16)
        primal = lax.map(solve_block, (blocks, right_side.reshape(slot_total // FDEV, FDEV, KKT, SC))).reshape(slot_total, KKT, SC)
        anchor = jnp.clip(primal, lower_limit[:, :, None], upper_limit[:, :, None])
        boundary = jnp.take_along_axis(primal, iface_rows[:, :, None], axis=1)
        outgoing = (boundary + scaled_dual) * active[:, None, None]
        summed = jax.ops.segment_sum(outgoing, substation_of, num_segments=S)
        new_consensus = (summed + reserve_weight[:, None, None] * reserve_target) / (members + reserve_weight)[:, None, None]
        dual_norm = penalty * jnp.sqrt(jnp.sum(members[:, None, None] * (new_consensus - consensus) ** 2))
        consensus = new_consensus
        local_consensus = consensus[substation_of]
        mismatch = boundary - local_consensus
        scaled_dual = (scaled_dual + mismatch) * active[:, None, None]
        primal_norm = jnp.sqrt(jnp.sum(active[:, None, None] * mismatch ** 2))
        history.append(jnp.stack([primal_norm, dual_norm]))
    return (penalty * scaled_dual, consensus, jnp.stack(history), anchor * active[:, None, None])
```

```python
import functools

import jax
import jax.numpy as jnp
from jax import lax
from jax.experimental import pallas as pl
from jax.experimental.pallas import tpu as pltpu
from jax.sharding import PartitionSpec as P

ITERS = 5
PENALTY = 2.0
LANES = 128
THIN = 16

f32 = jnp.float32
bf16 = jnp.bfloat16
i32 = jnp.int32


class Geometry:
    def __init__(self, slots, rows, ifc, scen, owned, n_sub, n_fdr):
        self.F, self.K, self.Q, self.C, self.S = slots, rows, ifc, scen, owned
        self.NB, self.G = n_sub, n_fdr
        self.D = n_sub * n_fdr
        overflow = max(1, slots // (2 * n_sub))
        cap = max(2, slots // n_sub + overflow)
        self.L = scen // n_fdr
        self.RP = n_fdr // 2
        self.R2 = -(-cap // self.RP)
        self.PR = self.R2 * self.RP
        self.Q2 = ifc // 2
        self.X = self.Q2 * self.R2
        self.stage_rows = self.G * self.X * self.NB
        self.id_lane = self.Q2 * self.PR * self.Q

    def off(self, q):
        q2, qp = divmod(q, 2)
        return (qp * self.RP * self.X + q2 * self.R2) * self.NB


def iota(shape, dim):
    return lax.broadcasted_iota(i32, shape, dim)


def group_mask(shape, g, width):
    lane = iota(shape, 1)
    return (lane >= g * width) & (lane < (g + 1) * width)


def roll(x, shift):
    shift = shift % LANES
    return pltpu.roll(x, shift, 1) if shift else x


def pack(geo, stage, send, chunk, off):
    n = geo.X * geo.NB
    for j in range(geo.G):
        acc = None
        for g in range(geo.G):
            v = roll(stage[g * n : (g + 1) * n, :], (g - j) * geo.L)
            acc = v if acc is None else jnp.where(group_mask((n, LANES), g, geo.L), v, acc)
        for x in range(geo.X):
            send[pl.ds(j * chunk + off + x, geo.NB, stride=geo.G * chunk), :] = acc[
                x * geo.NB : (x + 1) * geo.NB
            ]


def unpack(geo, recv, stage, chunk, off):
    n = geo.X * geo.NB
    parts = [
        jnp.concatenate(
            [
                recv[pl.ds(j * chunk + off + x, geo.NB, stride=geo.G * chunk), :]
                for x in range(geo.X)
            ],
            axis=0,
        )
        for j in range(geo.G)
    ]
    for g in range(geo.G):
        acc = None
        for j in range(geo.G):
            v = roll(parts[j], (j - g) * geo.L)
            acc = v if acc is None else jnp.where(group_mask((n, LANES), j, geo.L), v, acc)
        stage[g * n : (g + 1) * n, :] = acc


def dot(a, b):
    return jnp.dot(a, b, preferred_element_type=f32)


def limits(geo, lim, f):
    low = jnp.take_along_axis(lim[...], jnp.full((geo.K, LANES), f, i32), axis=1)
    high = jnp.take_along_axis(lim[...], jnp.full((geo.K, LANES), f + geo.F, i32), axis=1)
    return low, high


def feeder_first(geo, iface, sub, live, inverse, cost, lower, upper,
                 target, thin, lim, base, send, stage1, stage2, meta, count, rank):
    F, K, Q, NB, X = geo.F, geo.K, geo.Q, geo.NB, geo.X
    chunk = 2 * X + 2
    for k in range(NB):
        count[k] = 0

    def place(f, carry):
        k = lax.div(sub[f], geo.S)
        r = count[k]
        count[k] = r + 1
        rank[f] = r
        base[f] = (lax.rem(r, geo.RP) * X + lax.div(r, geo.RP)) * NB + k
        return carry

    lax.fori_loop(0, F, place, 0)
    stacked = jnp.concatenate(
        [lower[...], upper[...], jnp.zeros((LANES - 2 * F, K), f32)], axis=0
    )
    lim[...] = stacked.T
    stage1[...] = jnp.zeros_like(stage1)
    stage2[...] = jnp.zeros_like(stage2)
    meta[...] = jnp.zeros_like(meta)

    def body(f, carry):
        row = iota((THIN, K), 0)
        chosen = jnp.full((THIN, K), -1, i32)
        for q in range(Q):
            chosen = jnp.where(row == q, iface[f, q], chosen)
        hot = (iota((THIN, K), 1) == chosen).astype(f32).astype(bf16)
        full = inverse[f]
        few = dot(hot, full).astype(bf16)
        thin[f] = few
        c = cost[f]
        rhs = (-c).astype(bf16)
        primal = dot(full, rhs)
        h1 = dot(few, rhs)
        low, high = limits(geo, lim, f)
        t = jnp.minimum(jnp.maximum(primal, low), high) - c
        target[f] = t
        h2 = dot(few, t.astype(bf16))
        tall = jnp.concatenate([hot, jnp.zeros((LANES - THIN, K), bf16)], axis=0)
        square = lax.dot_general(few, tall, (((1,), (1,)), ((), ())), preferred_element_type=f32)
        r = rank[f]
        k = lax.div(sub[f], geo.S)
        square = pltpu.roll(square, r * Q, 1)
        row0 = jnp.zeros((1, LANES), f32)
        row1 = jnp.zeros((1, LANES), f32)
        for i in range(geo.Q2):
            moved = roll(square, i * geo.PR * Q)
            row0 = row0 + moved[i : i + 1]
            row1 = row1 + moved[geo.Q2 + i : geo.Q2 + i + 1]
        ident = jnp.where(f < live[0], sub[f] - k * geo.S + 1, 0).astype(f32)
        row0 = row0 + jnp.where(iota((1, LANES), 1) == geo.id_lane + r, ident, 0.0)
        meta[pl.ds(k, 1), :] = meta[pl.ds(k, 1), :] + row0
        meta[pl.ds(NB + k, 1), :] = meta[pl.ds(NB + k, 1), :] + row1
        at = base[f]
        for q in range(Q):
            stage1[pl.ds(at + geo.off(q), 1), :] = h1[q : q + 1]
            stage2[pl.ds(at + geo.off(q), 1), :] = h2[q : q + 1]
        return carry

    lax.fori_loop(0, F, body, 0)
    pack(geo, stage1, send, chunk, 0)
    pack(geo, stage2, send, chunk, X)
    for j in range(geo.G):
        for m in range(2):
            send[pl.ds(j * chunk + 2 * X + m, NB, stride=geo.G * chunk), :] = meta[
                m * NB : (m + 1) * NB
            ]


def solve(geo, f, iface, base, inverse, cost, lim, work, stage):
    at = base[f]
    for q in range(geo.Q):
        where = pl.ds(iface[f, q], 1)
        work[where, :] = work[where, :] + stage[pl.ds(at + geo.off(q), 1), :]
    primal = dot(inverse[f], work[...].astype(bf16))
    low, high = limits(geo, lim, f)
    return jnp.minimum(jnp.maximum(primal, low), high)


def feeder_steps(geo, steps, iface, base, inverse, cost, target, thin, lim, recv,
                 target_out, send, work, *stages):
    chunk_in = recv.shape[0] // geo.D
    chunk_out = steps * geo.X
    arrived, leaving = stages[:steps], stages[steps:]
    for s in range(steps):
        unpack(geo, recv, arrived[s], chunk_in, s * geo.X)
        leaving[s][...] = jnp.zeros_like(leaving[s])

    def body(f, carry):
        at = base[f]
        c = cost[f]
        work[...] = target[f]
        for s in range(steps):
            t = solve(geo, f, iface, base, inverse, cost, lim, work, arrived[s]) - c
            if s < steps - 1:
                work[...] = t
            h = dot(thin[f], t.astype(bf16))
            for q in range(geo.Q):
                leaving[s][pl.ds(at + geo.off(q), 1), :] = h[q : q + 1]
        target_out[f] = t
        return carry

    lax.fori_loop(0, geo.F, body, 0)
    for s in range(steps):
        pack(geo, leaving[s], send, chunk_out, s * geo.X)


def feeder_last(geo, iface, base, live, inverse, cost, target, lim, recv, out, work, stage):
    unpack(geo, recv, stage, recv.shape[0] // geo.D, geo.X)

    def body(f, carry):
        work[...] = target[f]
        anchor = solve(geo, f, iface, base, inverse, cost, lim, work, stage)
        out[f] = anchor * jnp.where(f < live[0], 1.0, 0.0)
        return carry

    lax.fori_loop(0, geo.F, body, 0)


def slice_parity(geo, shape):
    lane = iota(shape, 1)
    half = geo.RP * geo.L
    qp = jnp.where(lane >= half, 1, 0)
    inner = lane - qp * half
    rp = jnp.zeros(shape, i32)
    for i in range(1, geo.RP):
        rp = rp + jnp.where(inner >= i * geo.L, 1, 0)
    return qp, rp


def owner_setup(geo, slice_index, weight, aim, recv, coef, hot_t, hot, act, scaled, den, count):
    X, D, S, Q, Q2, R2, RP, PR = geo.X, geo.D, geo.S, geo.Q, geo.Q2, geo.R2, geo.RP, geo.PR
    chunk = 2 * X + 2
    metas = [recv[pl.ds(2 * X + m, D, stride=chunk), :] for m in range(2)]
    qp, rp = slice_parity(geo, (D, LANES))
    padded = metas[0]
    if D < LANES:
        padded = jnp.concatenate([padded, jnp.zeros((LANES - D, LANES), f32)], axis=0)
    turned = padded.T
    total = jnp.zeros((S, D), f32)
    for r2 in range(R2):
        live = jnp.zeros((D, LANES), f32)
        for p in range(RP):
            r = r2 * RP + p
            col = metas[0][:, geo.id_lane + r : geo.id_lane + r + 1]
            wide = jnp.broadcast_to(col, (D, LANES))
            live = jnp.where(rp == p, jnp.where(wide > 0.5, 1.0, 0.0), live)
            mine = (wide == (iota((D, LANES), 1) + 1).astype(f32)).astype(f32)
            hot[(p * R2 + r2) * D : (p * R2 + r2 + 1) * D, :] = mine[:, :S].astype(bf16)
            row = turned[geo.id_lane + r : geo.id_lane + r + 1, :D]
            theirs = (
                jnp.broadcast_to(row, (S, D)) == (iota((S, D), 0) + 1).astype(f32)
            ).astype(f32)
            total = total + theirs
            hot_t[r2, p * S : (p + 1) * S, :] = theirs.astype(bf16)
        act[r2 * D : (r2 + 1) * D, :] = live
    members = jnp.sum(total, axis=1, keepdims=True)
    w = jnp.zeros((S, LANES), f32)
    for s in range(S):
        w = jnp.where(iota((S, LANES), 0) == s, weight[s], w)
    members = jnp.broadcast_to(members, (S, LANES))
    den[...] = members + w
    qps, rps = slice_parity(geo, (S, LANES))
    count[...] = jnp.where(rps == 0, members, 0.0)
    lane = iota((S, LANES), 1)
    inner = lane - (qps * RP + rps) * geo.L
    index = inner + slice_index * geo.L
    for q2 in range(Q2):
        even = jnp.take_along_axis(aim[:, 2 * q2, :], index, axis=1)
        odd = jnp.take_along_axis(aim[:, 2 * q2 + 1, :], index, axis=1)
        scaled[:, q2 * LANES : (q2 + 1) * LANES] = w * jnp.where(qps == 0, even, odd)
    for par in range(2):
        for q2 in range(Q2):
            for q2p in range(Q2):
                for r2 in range(R2):
                    sides = []
                    for side in range(2):
                        q = 2 * q2 + side
                        other = 2 * q2p + (side if par == 0 else 1 - side)
                        sides.append((q // Q2, (q % Q2) * PR * Q + r2 * RP * Q + other))
                    idx = rp * Q + jnp.where(qp == 0, sides[0][1], sides[1][1])
                    if sides[0][0] == sides[1][0]:
                        value = jnp.take_along_axis(metas[sides[0][0]], idx, axis=1)
                    else:
                        value = jnp.where(
                            qp == 0,
                            jnp.take_along_axis(metas[sides[0][0]], idx, axis=1),
                            jnp.take_along_axis(metas[sides[1][0]], idx, axis=1),
                        )
                    coef[(par * Q2 + q2) * Q2 + q2p, r2 * D : (r2 + 1) * D, :] = value


def arrive(geo, recv, chunk, off):
    return [
        jnp.concatenate(
            [
                recv[pl.ds(off + q2 * geo.R2 + r2, geo.D, stride=chunk), :]
                for r2 in range(geo.R2)
            ],
            axis=0,
        )
        for q2 in range(geo.Q2)
    ]


def depart(geo, values, send, chunk, off):
    for q2 in range(geo.Q2):
        for r2 in range(geo.R2):
            send[pl.ds(off + q2 * geo.R2 + r2, geo.D, stride=chunk), :] = values[q2][
                r2 * geo.D : (r2 + 1) * geo.D
            ]


def split(x):
    high = x.astype(bf16)
    return high, (x - high.astype(f32)).astype(bf16)


def owner_step(geo, h, raised, dual, old, coef, hot_t, hot, act, scaled, den, count):
    D, S, Q2, R2, RP = geo.D, geo.S, geo.Q2, geo.R2, geo.RP
    n = R2 * D
    rows = list(h)
    if raised is not None:
        turned = [roll(v, geo.RP * geo.L) for v in raised]
        for q2 in range(Q2):
            acc = rows[q2]
            for q2p in range(Q2):
                acc = acc + coef[q2 * Q2 + q2p] * raised[q2p]
                acc = acc + coef[(Q2 + q2) * Q2 + q2p] * turned[q2p]
            rows[q2] = acc
    if dual is not None:
        rows = [b + u for b, u in zip(rows, dual)]
    high, low = split(jnp.concatenate(rows, axis=1))
    sums = None
    for r2 in range(R2):
        part = slice(r2 * D, (r2 + 1) * D)
        term = dot(hot_t[r2], high[part]) + dot(hot_t[r2], low[part])
        sums = term if sums is None else sums + term
    _, rps = slice_parity(geo, (S, LANES))
    fresh = []
    for q2 in range(Q2):
        cols = slice(q2 * LANES, (q2 + 1) * LANES)
        mine = sums[0:S, cols]
        for p in range(1, RP):
            mine = jnp.where(rps == p, sums[p * S : (p + 1) * S, cols], mine)
        whole = mine
        for s in range(1, RP):
            whole = whole + jnp.where(rps >= s, roll(mine, s * geo.L), 0.0)
            whole = whole + jnp.where(rps < RP - s, roll(mine, -s * geo.L), 0.0)
        fresh.append((whole + scaled[:, cols]) / den[...])
    high, low = split(jnp.concatenate(fresh, axis=1))
    back = dot(hot[...], high) + dot(hot[...], low)
    _, rpn = slice_parity(geo, (n, LANES))
    new_dual, new_raise = [], []
    moved = jnp.zeros((1, LANES), f32)
    for q2 in range(Q2):
        cols = slice(q2 * LANES, (q2 + 1) * LANES)
        own = back[0:n, cols]
        for p in range(1, RP):
            own = jnp.where(rpn == p, back[p * n : (p + 1) * n, cols], own)
        u = (rows[q2] - own) * act[...]
        new_dual.append(u)
        new_raise.append(PENALTY * (own - u))
        step = u if dual is None else u - dual[q2]
        moved = moved + jnp.sum(step * step, axis=0, keepdims=True)
    shifted = jnp.zeros((1, LANES), f32)
    for q2 in range(Q2):
        gap = fresh[q2] if old is None else fresh[q2] - old[q2]
        shifted = shifted + jnp.sum(count[...] * gap * gap, axis=0, keepdims=True)
    return new_dual, new_raise, fresh, moved, shifted


def read_list(geo, ref):
    return [ref[:, q2 * LANES : (q2 + 1) * LANES] for q2 in range(geo.Q2)]


def write_list(geo, ref, values):
    for q2 in range(geo.Q2):
        ref[:, q2 * LANES : (q2 + 1) * LANES] = values[q2]


def owner_first(geo, slice_index, weight, aim, recv,
                send, coef, hot_t, hot, act, scaled, den, count, dual, raised, old, norms):
    X = geo.X
    owner_setup(geo, slice_index[0], weight, aim, recv, coef, hot_t, hot, act, scaled, den, count)
    tables = (coef, hot_t, hot, act, scaled, den, count)
    chunk = 2 * X + 2
    h = arrive(geo, recv, chunk, 0)
    u, v, z, p0, d0 = owner_step(geo, h, None, None, None, *tables)
    depart(geo, v, send, 2 * X, 0)
    h = arrive(geo, recv, chunk, X)
    u, v, z, p1, d1 = owner_step(geo, h, v, u, z, *tables)
    depart(geo, v, send, 2 * X, X)
    write_list(geo, dual, u)
    write_list(geo, raised, v)
    write_list(geo, old, z)
    norms[...] = jnp.zeros_like(norms)
    for i, value in enumerate((p0, d0, p1, d1)):
        norms[i : i + 1] = value


def owner_middle(geo, first, recv, coef, hot_t, hot, act, scaled, den, count,
                 dual, raised, old, norms, send, dual_out, raised_out, old_out, norms_out):
    X = geo.X
    tables = (coef, hot_t, hot, act, scaled, den, count)
    u, v, z = read_list(geo, dual), read_list(geo, raised), read_list(geo, old)
    norms_out[...] = norms[...]
    for s in range(2):
        h = arrive(geo, recv, 2 * X, s * X)
        u, v, z, p, d = owner_step(geo, h, v, u, z, *tables)
        depart(geo, v, send, 2 * X, s * X)
        at = 2 * (first + s)
        norms_out[at : at + 1] = p
        norms_out[at + 1 : at + 2] = d
    write_list(geo, dual_out, u)
    write_list(geo, raised_out, v)
    write_list(geo, old_out, z)


def owner_last(geo, recv, coef, hot_t, hot, act, scaled, den, count,
               dual, raised, old, norms, send, agreed):
    X, S, RP = geo.X, geo.S, geo.RP
    tables = (coef, hot_t, hot, act, scaled, den, count)
    u, v, z = read_list(geo, dual), read_list(geo, raised), read_list(geo, old)
    h = arrive(geo, recv, X, 0)
    u, v, z, p, d = owner_step(geo, h, v, u, z, *tables)
    depart(geo, [PENALTY * x for x in u], send, X + 1, 0)
    at = 2 * (ITERS - 1)
    everything = norms[...]
    rows = everything.shape[0]
    row = iota((rows, LANES), 0)
    everything = jnp.where(row == at, p, everything)
    everything = jnp.where(row == at + 1, d, everything)
    sums = jnp.sum(everything, axis=1, keepdims=True)
    line = jnp.sum(jnp.where(row == iota((rows, LANES), 1), sums, 0.0), axis=0, keepdims=True)
    send[pl.ds(X, geo.D, stride=X + 1), :] = jnp.broadcast_to(line, (geo.D, LANES))
    part = S // RP
    _, rps = slice_parity(geo, (part, LANES))
    for q2 in range(geo.Q2):
        value = z[q2][0:part]
        for i in range(1, RP):
            value = jnp.where(rps == i, z[q2][i * part : (i + 1) * part], value)
        agreed[q2 * part : (q2 + 1) * part, :] = value


def finish(geo, base, recv, agreed, duals, consensus, norms, stage):
    X, S, RP, G, L = geo.X, geo.S, geo.RP, geo.G, geo.L
    unpack(geo, recv, stage, X + 1, 0)

    def body(f, carry):
        at = base[f]
        for q in range(geo.Q):
            duals[f, q : q + 1, :] = stage[pl.ds(at + geo.off(q), 1), :]
        return carry

    lax.fori_loop(0, geo.F, body, 0)
    part = S // RP
    n = geo.Q2 * part
    for q2 in range(geo.Q2):
        sides = [agreed[j * n + q2 * part : j * n + (q2 + 1) * part, :] for j in range(G)]
        for qp in range(2):
            for rp in range(RP):
                acc = None
                for j in range(G):
                    v = roll(sides[j], (j - (qp * RP + rp)) * L)
                    acc = v if acc is None else jnp.where(group_mask((part, LANES), j, L), v, acc)
                consensus[rp * part : (rp + 1) * part, 2 * q2 + qp, :] = acc
    line = jnp.sum(recv[pl.ds(X, geo.D, stride=X + 1), :], axis=0, keepdims=True)
    line = jnp.sqrt(line)
    lane = iota((8, LANES), 1)
    wide = jnp.broadcast_to(line, (8, LANES))
    table = jnp.zeros((8, LANES), f32)
    for i in range(ITERS):
        table = jnp.where(iota((8, LANES), 0) == i, roll(wide, -2 * i), table)
    table = jnp.where(lane == 1, PENALTY * table, table)
    norms[...] = table[:ITERS, :2]


VM = pltpu.VMEM
SM = pltpu.SMEM


def call(body, args, ins, outs, scratch=(), name=None):
    specs = [pl.BlockSpec(memory_space=s) for s in ins]
    return pl.pallas_call(
        body,
        in_specs=specs,
        out_specs=[pl.BlockSpec(memory_space=s) for _, _, s in outs],
        out_shape=[jax.ShapeDtypeStruct(shape, dtype) for shape, dtype, _ in outs],
        scratch_shapes=list(scratch),
        compiler_params=pltpu.CompilerParams(vmem_limit_bytes=40 << 20),
        name=name,
    )(*args)


def shards(
    n_sub,
    n_fdr,
    inverse,
    cost,
    lower_limit,
    upper_limit,
    iface_rows,
    substation_of,
    live_count,
    reserve_weight,
    reserve_target,
):
    slots, rows, scen = cost.shape
    geo = Geometry(slots, rows, iface_rows.shape[1], scen, reserve_weight.shape[0], n_sub, n_fdr)
    F, K, Q, C, S, D, X = geo.F, geo.K, geo.Q, geo.C, geo.S, geo.D, geo.X
    R2, RP, Q2 = geo.R2, geo.RP, geo.Q2
    n, wide = R2 * D, Q2 * LANES

    def swap(x):
        y = x.reshape(D, 1, x.shape[0] // D * LANES)
        y = lax.all_to_all(y, ("sub", "fdr"), split_axis=0, concat_axis=0, tiled=True)
        return y.reshape(x.shape)

    stage = pltpu.VMEM((geo.stage_rows, LANES), f32)
    work = pltpu.VMEM((K, LANES), f32)
    slice_index = lax.axis_index("fdr").astype(i32).reshape(1)

    target, thin, lim, base, send = call(
        functools.partial(feeder_first, geo),
        (iface_rows, substation_of, live_count, inverse, cost, lower_limit, upper_limit),
        (SM, SM, SM, VM, VM, VM, VM),
        (
            ((F, K, C), f32, VM),
            ((F, THIN, K), bf16, VM),
            ((K, LANES), f32, VM),
            ((F,), i32, SM),
            ((D * (2 * X + 2), LANES), f32, VM),
        ),
        (stage, stage, pltpu.VMEM((2 * geo.NB, LANES), f32), pltpu.SMEM((geo.NB,), i32),
         pltpu.SMEM((F,), i32)),
        "feeder_first",
    )
    state = (
        ((n, wide), f32, VM),
        ((n, wide), f32, VM),
        ((S, wide), f32, VM),
        ((16, LANES), f32, VM),
    )
    out = call(
        functools.partial(owner_first, geo),
        (slice_index, reserve_weight, reserve_target, swap(send)),
        (SM, SM, VM, VM),
        (
            ((D * 2 * X, LANES), f32, VM),
            ((2 * Q2 * Q2, n, LANES), f32, VM),
            ((R2, RP * S, D), bf16, VM),
            ((RP * n, S), bf16, VM),
            ((n, LANES), f32, VM),
            ((S, wide), f32, VM),
            ((S, LANES), f32, VM),
            ((S, LANES), f32, VM),
        )
        + state,
        (),
        "owner_first",
    )
    send, tables, memory = out[0], out[1:8], out[8:]
    for first in range(2, ITERS - 1, 2):
        recv = swap(send)
        target, send = call(
            functools.partial(feeder_steps, geo, 2),
            (iface_rows, base, inverse, cost, target, thin, lim, recv),
            (SM, SM, VM, VM, VM, VM, VM, VM),
            (((F, K, C), f32, VM), ((D * 2 * X, LANES), f32, VM)),
            (work, stage, stage, stage, stage),
            "feeder_steps",
        )
        out = call(
            functools.partial(owner_middle, geo, first),
            (swap(send), *tables, *memory),
            (VM,) * 12,
            (((D * 2 * X, LANES), f32, VM),) + state,
            (),
            "owner_middle",
        )
        send, memory = out[0], out[1:]
    recv = swap(send)
    target, send = call(
        functools.partial(feeder_steps, geo, 1),
        (iface_rows, base, inverse, cost, target, thin, lim, recv),
        (SM, SM, VM, VM, VM, VM, VM, VM),
        (((F, K, C), f32, VM), ((D * X, LANES), f32, VM)),
        (work, stage, stage),
        "feeder_ahead",
    )
    (setpoints,) = call(
        functools.partial(feeder_last, geo),
        (iface_rows, base, live_count, inverse, cost, target, lim, recv),
        (SM, SM, SM, VM, VM, VM, VM, VM),
        (((F, K, C), f32, VM),),
        (work, stage),
        "feeder_last",
    )
    send, agreed = call(
        functools.partial(owner_last, geo),
        (swap(send), *tables, *memory),
        (VM,) * 12,
        (((D * (X + 1), LANES), f32, VM), ((Q2 * S // RP, LANES), f32, VM)),
        (),
        "owner_last",
    )
    gathered = lax.all_gather(agreed, "fdr", axis=0, tiled=True)
    duals, consensus, norms = call(
        functools.partial(finish, geo),
        (base, swap(send), gathered),
        (SM, VM, VM),
        (((F, Q, C), f32, VM), ((S, Q, C), f32, VM), ((ITERS, 2), f32, VM)),
        (stage,),
        "finish",
    )
    return duals, consensus, norms, setpoints


def solution(mesh):
    placed = (
        P(("sub", "fdr"), None, None),
        P(("sub", "fdr"), None, None),
        P(("sub", "fdr"), None),
        P(("sub", "fdr"), None),
        P(("sub", "fdr"), None),
        P(("sub", "fdr")),
        P(("sub", "fdr")),
        P("sub"),
        P("sub", None, None),
    )
    return jax.shard_map(
        functools.partial(shards, mesh.shape["sub"], mesh.shape["fdr"]),
        mesh=mesh,
        in_specs=placed,
        out_specs=(
            P(("sub", "fdr"), None, None),
            P("sub", None, None),
            P(),
            P(("sub", "fdr"), None, None),
        ),
        check_vma=False,
    )
```

```python
import functools

import jax
import jax.numpy as jnp
from jax import lax
from jax.experimental import pallas as pl
from jax.experimental.pallas import tpu as pltpu
from jax.sharding import PartitionSpec as P

ITERS = 5
PENALTY = 2.0
LANES = 128
THIN = 16
GROUP = 4

f32 = jnp.float32
bf16 = jnp.bfloat16
i32 = jnp.int32


class Geometry:
    def __init__(self, slots, rows, ifc, scen, owned, n_sub, n_fdr):
        self.F, self.K, self.Q, self.C, self.S = slots, rows, ifc, scen, owned
        self.NB, self.G = n_sub, n_fdr
        self.D = n_sub * n_fdr
        overflow = max(1, slots // (2 * n_sub))
        cap = max(2, slots // n_sub + overflow)
        self.L = scen // n_fdr
        self.RP = n_fdr // 2
        self.R2 = -(-cap // self.RP)
        self.PR = self.R2 * self.RP
        self.Q2 = ifc // 2
        self.X = self.Q2 * self.R2
        self.stage_rows = self.G * self.X * self.NB
        self.id_lane = self.Q2 * self.PR * self.Q

    def off(self, q):
        q2, qp = divmod(q, 2)
        return (qp * self.RP * self.X + q2 * self.R2) * self.NB


def iota(shape, dim):
    return lax.broadcasted_iota(i32, shape, dim)


def group_mask(shape, g, width):
    lane = iota(shape, 1)
    return (lane >= g * width) & (lane < (g + 1) * width)


def roll(x, shift):
    shift = shift % LANES
    return pltpu.roll(x, shift, 1) if shift else x


def pack(geo, stage, send, chunk, off):
    n = geo.X * geo.NB
    for j in range(geo.G):
        acc = None
        for g in range(geo.G):
            v = roll(stage[g * n : (g + 1) * n, :], (g - j) * geo.L)
            acc = v if acc is None else jnp.where(group_mask((n, LANES), g, geo.L), v, acc)
        for x in range(geo.X):
            send[pl.ds(j * chunk + off + x, geo.NB, stride=geo.G * chunk), :] = acc[
                x * geo.NB : (x + 1) * geo.NB
            ]


def unpack(geo, recv, stage, chunk, off):
    n = geo.X * geo.NB
    parts = [
        jnp.concatenate(
            [
                recv[pl.ds(j * chunk + off + x, geo.NB, stride=geo.G * chunk), :]
                for x in range(geo.X)
            ],
            axis=0,
        )
        for j in range(geo.G)
    ]
    for g in range(geo.G):
        acc = None
        for j in range(geo.G):
            v = roll(parts[j], (j - g) * geo.L)
            acc = v if acc is None else jnp.where(group_mask((n, LANES), j, geo.L), v, acc)
        stage[g * n : (g + 1) * n, :] = acc


def dot(a, b):
    return jnp.dot(a, b, preferred_element_type=f32)


def limits(geo, lim, f):
    table = lim[...]
    low = jnp.take_along_axis(table, jnp.full((geo.K, LANES), f, i32), axis=1)
    high = jnp.take_along_axis(table, jnp.full((geo.K, LANES), f + geo.F, i32), axis=1)
    return low, high


def clip(x, low, high):
    return jnp.minimum(jnp.maximum(x, low), high)


def moves(pairs, sems, group):
    count = pairs[0][0].shape[0] // group

    def one(i, c):
        src, dst = pairs[i]
        part = pl.ds(c * group, group)
        return pltpu.make_async_copy(src.at[part], dst.at[part], sems.at[i, c])

    return count, one


def pick(work, iface, f, q):
    return work[pl.ds(iface[q, f], 1), :]


def feeder_first(geo, iface, sub, live, inverse, cost, lower, upper,
                 rounded, kept, lim, base, send,
                 inv, price, out, sems, out_sems,
                 stage1, stage2, meta, count, rank, *works):
    F, K, Q, NB, X = geo.F, geo.K, geo.Q, geo.NB, geo.X
    chunk = 2 * X + 2
    bound, square, left, ahead = (works[i * GROUP : (i + 1) * GROUP] for i in range(4))
    groups, load = moves(((inverse, inv), (cost, price)), sems, GROUP)
    _, store = moves(((out, rounded),), out_sems, GROUP)
    for c in range(groups):
        for i in range(2):
            load(i, c).start()
    for k in range(NB):
        count[k] = 0

    def place(f, carry):
        k = lax.div(sub[f], geo.S)
        r = count[k]
        count[k] = r + 1
        rank[f] = r
        base[f] = (lax.rem(r, geo.RP) * X + lax.div(r, geo.RP)) * NB + k
        return carry

    lax.fori_loop(0, F, place, 0)
    stacked = jnp.concatenate(
        [lower[...], upper[...], jnp.zeros((LANES - 2 * F, K), f32)], axis=0
    )
    lim[...] = stacked.T
    stage1[...] = jnp.zeros_like(stage1)
    stage2[...] = jnp.zeros_like(stage2)
    meta[...] = jnp.zeros_like(meta)
    kept[...] = jnp.zeros_like(kept)
    lane = iota((1, LANES), 1)
    third = jnp.zeros((1, LANES), i32)
    for i in range(1, geo.Q2 + 1):
        third = third + jnp.where(lane >= i * geo.PR * Q, 1, 0)
    within = lane - third * (geo.PR * Q)

    def body(c, carry):
        for i in range(2):
            load(i, c).wait()
        fs = [c * GROUP + u for u in range(GROUP)]
        for u, f in enumerate(fs):
            at = within - rank[f] * Q
            chosen = jnp.full((1, LANES), -1, i32)
            for q in range(Q):
                chosen = jnp.where((at == q) & (third < geo.Q2), iface[q, f], chosen)
            hot = (iota((K, LANES), 0) == jnp.broadcast_to(chosen, (K, LANES))).astype(f32)
            price_u = price[f]
            both = dot(inv[f], jnp.concatenate([-price_u, hot], axis=1).astype(bf16))
            primal = both[:, :LANES]
            bound[u][...] = primal
            square[u][...] = both[:, LANES:]
            low, high = limits(geo, lim, f)
            t = clip(primal, low, high) - price_u
            left[u][...] = t
            t = t.astype(bf16)
            out[f] = t
            ahead[u][...] = dot(inv[f], t)
        store(0, c).start()
        for u, f in enumerate(fs):
            k = lax.div(sub[f], geo.S)
            ident = jnp.where(f < live[0], sub[f] - k * geo.S + 1, 0).astype(f32)
            lines = [jnp.where(lane == geo.id_lane + rank[f], ident, 0.0),
                     jnp.zeros((1, LANES), f32)]
            at = base[f]
            for q in range(Q):
                m, i = divmod(q, geo.Q2)
                lines[m] = lines[m] + jnp.where(third == i, pick(square[u], iface, f, q), 0.0)
                stage1[pl.ds(at + geo.off(q), 1), :] = pick(bound[u], iface, f, q)
                stage2[pl.ds(at + geo.off(q), 1), :] = pick(ahead[u], iface, f, q)
                kept[f, q : q + 1, :] = pick(left[u], iface, f, q)
            for m in range(2):
                spot = pl.ds(m * NB + k, 1)
                meta[spot, :] = meta[spot, :] + lines[m]
        return carry

    lax.fori_loop(0, groups, body, 0)
    pack(geo, stage1, send, chunk, 0)
    pack(geo, stage2, send, chunk, X)
    for j in range(geo.G):
        for m in range(2):
            send[pl.ds(j * chunk + 2 * X + m, NB, stride=geo.G * chunk), :] = meta[
                m * NB : (m + 1) * NB
            ]
    for c in range(groups):
        store(0, c).wait()


def raise_rows(geo, f, iface, base, rows, work, stage):
    at = base[f]
    rows = [rows[q] + stage[pl.ds(at + geo.off(q), 1), :] for q in range(geo.Q)]
    for q in range(geo.Q):
        work[pl.ds(iface[q, f], 1), :] = rows[q]


def feeder_pair(geo, last, iface, base, live, inverse, cost, rounded, kept, lim, recv, *rest):
    if last:
        result, send, inv, price, held, out, sems, out_sems = rest[:8]
        rest = rest[8:]
    else:
        result, kept_out, send, inv, price, held, out, sems, out_sems = rest[:9]
        rest = rest[9:]
    ways = 1 if last else 2
    arrived, leaving, works = rest[:2], rest[2 : 2 + ways], rest[2 + ways :]
    side, bound, left, ahead = (works[i * GROUP : (i + 1) * GROUP] for i in range(4))
    groups, load = moves(((inverse, inv), (cost, price), (rounded, held)), sems, GROUP)
    _, store = moves(((out, result),), out_sems, GROUP)
    for c in range(groups):
        for i in range(3):
            load(i, c).start()
    for s in range(2):
        unpack(geo, recv, arrived[s], 2 * geo.X, s * geo.X)
    for stage in leaving:
        stage[...] = jnp.zeros_like(stage)
    if not last:
        kept_out[...] = jnp.zeros_like(kept_out)

    def body(c, carry):
        for i in range(3):
            load(i, c).wait()
        fs = [c * GROUP + u for u in range(GROUP)]
        for u, f in enumerate(fs):
            side[u][...] = held[f].astype(f32)
            rows = [kept[f, q : q + 1, :] for q in range(geo.Q)]
            raise_rows(geo, f, iface, base, rows, side[u], arrived[0])
        for u, f in enumerate(fs):
            low, high = limits(geo, lim, f)
            left[u][...] = clip(dot(inv[f], side[u][...].astype(bf16)), low, high) - price[f]
        for u, f in enumerate(fs):
            rows = [pick(left[u], iface, f, q) for q in range(geo.Q)]
            raise_rows(geo, f, iface, base, rows, left[u], arrived[1])
        for u, f in enumerate(fs):
            low, high = limits(geo, lim, f)
            primal = dot(inv[f], left[u][...].astype(bf16))
            bound[u][...] = primal
            anchor = clip(primal, low, high)
            if last:
                out[f] = anchor * jnp.where(f < live[0], 1.0, 0.0)
            else:
                t = anchor - price[f]
                side[u][...] = t
                t = t.astype(bf16)
                out[f] = t
                ahead[u][...] = dot(inv[f], t)
        store(0, c).start()
        for u, f in enumerate(fs):
            at = base[f]
            for q in range(geo.Q):
                leaving[0][pl.ds(at + geo.off(q), 1), :] = pick(bound[u], iface, f, q)
                if not last:
                    leaving[1][pl.ds(at + geo.off(q), 1), :] = pick(ahead[u], iface, f, q)
                    kept_out[f, q : q + 1, :] = pick(side[u], iface, f, q)
        return carry

    lax.fori_loop(0, groups, body, 0)
    for s in range(ways):
        pack(geo, leaving[s], send, ways * geo.X, s * geo.X)
    for c in range(groups):
        store(0, c).wait()


def slice_parity(geo, shape):
    lane = iota(shape, 1)
    half = geo.RP * geo.L
    qp = jnp.where(lane >= half, 1, 0)
    inner = lane - qp * half
    rp = jnp.zeros(shape, i32)
    for i in range(1, geo.RP):
        rp = rp + jnp.where(inner >= i * geo.L, 1, 0)
    return qp, rp


def owner_setup(geo, slice_index, weight, aim, recv, coef, hot_t, hot, act, scaled, den, count):
    X, D, S, Q, Q2, R2, RP, PR = geo.X, geo.D, geo.S, geo.Q, geo.Q2, geo.R2, geo.RP, geo.PR
    chunk = 2 * X + 2
    metas = [recv[pl.ds(2 * X + m, D, stride=chunk), :] for m in range(2)]
    qp, rp = slice_parity(geo, (D, LANES))
    padded = metas[0]
    if D < LANES:
        padded = jnp.concatenate([padded, jnp.zeros((LANES - D, LANES), f32)], axis=0)
    turned = padded.T
    total = jnp.zeros((S, D), f32)
    for r2 in range(R2):
        live = jnp.zeros((D, LANES), f32)
        for p in range(RP):
            r = r2 * RP + p
            col = metas[0][:, geo.id_lane + r : geo.id_lane + r + 1]
            wide = jnp.broadcast_to(col, (D, LANES))
            live = jnp.where(rp == p, jnp.where(wide > 0.5, 1.0, 0.0), live)
            mine = (wide == (iota((D, LANES), 1) + 1).astype(f32)).astype(f32)
            hot[(p * R2 + r2) * D : (p * R2 + r2 + 1) * D, :] = mine[:, :S].astype(bf16)
            row = turned[geo.id_lane + r : geo.id_lane + r + 1, :D]
            theirs = (
                jnp.broadcast_to(row, (S, D)) == (iota((S, D), 0) + 1).astype(f32)
            ).astype(f32)
            total = total + theirs
            hot_t[r2, p * S : (p + 1) * S, :] = theirs.astype(bf16)
        act[r2 * D : (r2 + 1) * D, :] = live
    members = jnp.sum(total, axis=1, keepdims=True)
    w = jnp.zeros((S, LANES), f32)
    for s in range(S):
        w = jnp.where(iota((S, LANES), 0) == s, weight[s], w)
    members = jnp.broadcast_to(members, (S, LANES))
    den[...] = members + w
    qps, rps = slice_parity(geo, (S, LANES))
    count[...] = jnp.where(rps == 0, members, 0.0)
    lane = iota((S, LANES), 1)
    inner = lane - (qps * RP + rps) * geo.L
    index = inner + slice_index * geo.L
    for q2 in range(Q2):
        even = jnp.take_along_axis(aim[2 * q2], index, axis=1)
        odd = jnp.take_along_axis(aim[2 * q2 + 1], index, axis=1)
        scaled[:, q2 * LANES : (q2 + 1) * LANES] = w * jnp.where(qps == 0, even, odd)
    for par in range(2):
        for q2 in range(Q2):
            for q2p in range(Q2):
                for r2 in range(R2):
                    sides = []
                    for side in range(2):
                        q = 2 * q2 + side
                        other = 2 * q2p + (side if par == 0 else 1 - side)
                        sides.append((q // Q2, (q % Q2) * PR * Q + r2 * RP * Q + other))
                    idx = rp * Q + jnp.where(qp == 0, sides[0][1], sides[1][1])
                    if sides[0][0] == sides[1][0]:
                        value = jnp.take_along_axis(metas[sides[0][0]], idx, axis=1)
                    else:
                        value = jnp.where(
                            qp == 0,
                            jnp.take_along_axis(metas[sides[0][0]], idx, axis=1),
                            jnp.take_along_axis(metas[sides[1][0]], idx, axis=1),
                        )
                    coef[(par * Q2 + q2) * Q2 + q2p, r2 * D : (r2 + 1) * D, :] = value


def arrive(geo, recv, chunk, off):
    return [
        jnp.concatenate(
            [
                recv[pl.ds(off + q2 * geo.R2 + r2, geo.D, stride=chunk), :]
                for r2 in range(geo.R2)
            ],
            axis=0,
        )
        for q2 in range(geo.Q2)
    ]


def depart(geo, values, send, chunk, off):
    for q2 in range(geo.Q2):
        for r2 in range(geo.R2):
            send[pl.ds(off + q2 * geo.R2 + r2, geo.D, stride=chunk), :] = values[q2][
                r2 * geo.D : (r2 + 1) * geo.D
            ]


def split(x):
    high = x.astype(bf16)
    return high, (x - high.astype(f32)).astype(bf16)


def owner_step(geo, h, raised, dual, old, coef, hot_t, hot, act, scaled, den, count):
    D, S, Q2, R2, RP = geo.D, geo.S, geo.Q2, geo.R2, geo.RP
    n = R2 * D
    rows = list(h)
    if raised is not None:
        turned = [roll(v, geo.RP * geo.L) for v in raised]
        for q2 in range(Q2):
            acc = rows[q2]
            for q2p in range(Q2):
                acc = acc + coef[q2 * Q2 + q2p] * raised[q2p]
                acc = acc + coef[(Q2 + q2) * Q2 + q2p] * turned[q2p]
            rows[q2] = acc
    if dual is not None:
        rows = [b + u for b, u in zip(rows, dual)]
    high, low = split(jnp.concatenate(rows, axis=1))
    sums = None
    for r2 in range(R2):
        part = slice(r2 * D, (r2 + 1) * D)
        term = dot(hot_t[r2], high[part]) + dot(hot_t[r2], low[part])
        sums = term if sums is None else sums + term
    _, rps = slice_parity(geo, (S, LANES))
    fresh = []
    for q2 in range(Q2):
        cols = slice(q2 * LANES, (q2 + 1) * LANES)
        mine = sums[0:S, cols]
        for p in range(1, RP):
            mine = jnp.where(rps == p, sums[p * S : (p + 1) * S, cols], mine)
        whole = mine
        for s in range(1, RP):
            whole = whole + jnp.where(rps >= s, roll(mine, s * geo.L), 0.0)
            whole = whole + jnp.where(rps < RP - s, roll(mine, -s * geo.L), 0.0)
        fresh.append((whole + scaled[:, cols]) / den[...])
    high, low = split(jnp.concatenate(fresh, axis=1))
    back = dot(hot[...], high) + dot(hot[...], low)
    _, rpn = slice_parity(geo, (n, LANES))
    new_dual, new_raise = [], []
    moved = jnp.zeros((1, LANES), f32)
    for q2 in range(Q2):
        cols = slice(q2 * LANES, (q2 + 1) * LANES)
        own = back[0:n, cols]
        for p in range(1, RP):
            own = jnp.where(rpn == p, back[p * n : (p + 1) * n, cols], own)
        u = (rows[q2] - own) * act[...]
        new_dual.append(u)
        new_raise.append(PENALTY * (own - u))
        step = u if dual is None else u - dual[q2]
        moved = moved + jnp.sum(step * step, axis=0, keepdims=True)
    shifted = jnp.zeros((1, LANES), f32)
    for q2 in range(Q2):
        gap = fresh[q2] if old is None else fresh[q2] - old[q2]
        shifted = shifted + jnp.sum(count[...] * gap * gap, axis=0, keepdims=True)
    return new_dual, new_raise, fresh, moved, shifted


def read_list(geo, ref):
    return [ref[:, q2 * LANES : (q2 + 1) * LANES] for q2 in range(geo.Q2)]


def write_list(geo, ref, values):
    for q2 in range(geo.Q2):
        ref[:, q2 * LANES : (q2 + 1) * LANES] = values[q2]


def owner_first(geo, slice_index, weight, aim, recv,
                send, coef, hot_t, hot, act, scaled, den, count, dual, old, norms):
    X = geo.X
    owner_setup(geo, slice_index[0], weight, aim, recv, coef, hot_t, hot, act, scaled, den, count)
    tables = (coef, hot_t, hot, act, scaled, den, count)
    chunk = 2 * X + 2
    h = arrive(geo, recv, chunk, 0)
    u, v, z, p0, d0 = owner_step(geo, h, None, None, None, *tables)
    depart(geo, v, send, 2 * X, 0)
    h = arrive(geo, recv, chunk, X)
    u, v, z, p1, d1 = owner_step(geo, h, v, u, z, *tables)
    depart(geo, v, send, 2 * X, X)
    write_list(geo, dual, u)
    write_list(geo, old, z)
    norms[...] = jnp.zeros_like(norms)
    for i, value in enumerate((p0, d0, p1, d1)):
        norms[i : i + 1] = value


def owner_middle(geo, first, recv, coef, hot_t, hot, act, scaled, den, count,
                 dual, old, norms, send, dual_out, old_out, norms_out):
    X = geo.X
    tables = (coef, hot_t, hot, act, scaled, den, count)
    u, v, z = read_list(geo, dual), None, read_list(geo, old)
    norms_out[...] = norms[...]
    for s in range(2):
        h = arrive(geo, recv, 2 * X, s * X)
        u, v, z, p, d = owner_step(geo, h, v if s else None, u, z, *tables)
        depart(geo, v, send, 2 * X, s * X)
        at = 2 * (first + s)
        norms_out[at : at + 1] = p
        norms_out[at + 1 : at + 2] = d
    write_list(geo, dual_out, u)
    write_list(geo, old_out, z)


def owner_last(geo, recv, coef, hot_t, hot, act, scaled, den, count,
               dual, old, norms, send, agreed):
    X, S, RP = geo.X, geo.S, geo.RP
    tables = (coef, hot_t, hot, act, scaled, den, count)
    u, v, z = read_list(geo, dual), None, read_list(geo, old)
    h = arrive(geo, recv, X, 0)
    u, v, z, p, d = owner_step(geo, h, None, u, z, *tables)
    depart(geo, [PENALTY * x for x in u], send, X + 1, 0)
    at = 2 * (ITERS - 1)
    everything = norms[...]
    rows = everything.shape[0]
    row = iota((rows, LANES), 0)
    everything = jnp.where(row == at, p, everything)
    everything = jnp.where(row == at + 1, d, everything)
    sums = jnp.sum(everything, axis=1, keepdims=True)
    line = jnp.sum(jnp.where(row == iota((rows, LANES), 1), sums, 0.0), axis=0, keepdims=True)
    send[pl.ds(X, geo.D, stride=X + 1), :] = jnp.broadcast_to(line, (geo.D, LANES))
    part = S // RP
    _, rps = slice_parity(geo, (part, LANES))
    for q2 in range(geo.Q2):
        value = z[q2][0:part]
        for i in range(1, RP):
            value = jnp.where(rps == i, z[q2][i * part : (i + 1) * part], value)
        agreed[q2 * part : (q2 + 1) * part, :] = value


def finish(geo, base, recv, agreed, duals, consensus, norms, stage):
    X, S, RP, G, L = geo.X, geo.S, geo.RP, geo.G, geo.L
    unpack(geo, recv, stage, X + 1, 0)

    def body(f, carry):
        at = base[f]
        for q in range(geo.Q):
            duals[q, pl.ds(f, 1), :] = stage[pl.ds(at + geo.off(q), 1), :]
        return carry

    lax.fori_loop(0, geo.F, body, 0)
    part = S // RP
    n = geo.Q2 * part
    for q2 in range(geo.Q2):
        sides = [agreed[j * n + q2 * part : j * n + (q2 + 1) * part, :] for j in range(G)]
        for qp in range(2):
            for rp in range(RP):
                acc = None
                for j in range(G):
                    v = roll(sides[j], (j - (qp * RP + rp)) * L)
                    acc = v if acc is None else jnp.where(group_mask((part, LANES), j, L), v, acc)
                consensus[2 * q2 + qp, rp * part : (rp + 1) * part, :] = acc
    line = jnp.sum(recv[pl.ds(X, geo.D, stride=X + 1), :], axis=0, keepdims=True)
    line = jnp.broadcast_to(jnp.sqrt(line), (8, LANES))
    side = iota((8, LANES), 0)
    lane = iota((8, LANES), 1)
    table = jnp.zeros((8, LANES), f32)
    for i in range(ITERS):
        table = jnp.where((lane == i) & (side == 0), roll(line, -i), table)
        table = jnp.where((lane == i) & (side == 1), PENALTY * roll(line, -i - 1), table)
    norms[...] = table[:2, :ITERS]


VM = pltpu.VMEM
SM = pltpu.SMEM
HB = pltpu.HBM


def call(body, args, ins, outs, scratch=(), name=None):
    args = [
        pltpu.with_memory_space_constraint(x, HB) if s is HB else x for x, s in zip(args, ins)
    ]
    return pl.pallas_call(
        body,
        in_specs=[pl.BlockSpec(memory_space=s) for s in ins],
        out_specs=[pl.BlockSpec(memory_space=s) for _, _, s in outs],
        out_shape=[
            jax.ShapeDtypeStruct(shape, dtype) if s is VM else s(shape, dtype)
            for shape, dtype, s in outs
        ],
        scratch_shapes=list(scratch),
        compiler_params=pltpu.CompilerParams(vmem_limit_bytes=40 << 20),
        name=name,
    )(*args)


def feeder_calls(geo, iface, substation_of, live_count, inverse, cost, lower, upper):
    F, K, C, D, X = geo.F, geo.K, geo.C, geo.D, geo.X
    groups = F // GROUP
    stage = pltpu.VMEM((geo.stage_rows, LANES), f32)
    works = (pltpu.VMEM((K, LANES), f32),) * (4 * GROUP)
    squares = pltpu.VMEM((F, K, K), bf16)
    prices = pltpu.VMEM((F, K, C), f32)
    halves = pltpu.VMEM((F, K, C), bf16)
    carried = (((F, K, C), bf16, HB), ((F, 8, C), f32, VM))

    def sems(count):
        return pltpu.SemaphoreType.DMA((count, groups))

    def begin():
        rounded, kept, lim, base, send = call(
            functools.partial(feeder_first, geo),
            (iface, substation_of, live_count, inverse, cost, lower, upper),
            (SM, SM, SM, HB, HB, VM, VM),
            carried
            + (
                ((K, LANES), f32, VM),
                ((F,), i32, SM),
                ((D * (2 * X + 2), LANES), f32, VM),
            ),
            (squares, prices, halves, sems(2), sems(1),
             stage, stage, pltpu.VMEM((2 * geo.NB, LANES), f32), pltpu.SMEM((geo.NB,), i32),
             pltpu.SMEM((F,), i32)) + works,
            "feeder_first",
        )
        return (rounded, kept, lim, base), base, send

    def advance(state, recv, last):
        rounded, kept, lim, base = state
        out = call(
            functools.partial(feeder_pair, geo, last),
            (iface, base, live_count, inverse, cost, rounded, kept, lim, recv),
            (SM, SM, SM, HB, HB, HB, VM, VM, VM),
            ((((F, K, C), f32, HB),) if last else carried)
            + (((D * (1 if last else 2) * X, LANES), f32, VM),),
            (squares, prices, halves, prices if last else halves, sems(3), sems(1))
            + (stage,) * (3 if last else 4) + works,
            "feeder_last" if last else "feeder_pair",
        )
        return out if last else ((out[0], out[1], lim, base), out[2])

    return begin, advance


def shards(
    n_sub,
    n_fdr,
    inverse,
    cost,
    lower_limit,
    upper_limit,
    iface_rows,
    substation_of,
    live_count,
    reserve_weight,
    reserve_target,
):
    slots, rows, scen = cost.shape
    geo = Geometry(slots, rows, iface_rows.shape[1], scen, reserve_weight.shape[0], n_sub, n_fdr)
    F, K, Q, C, S, D, X = geo.F, geo.K, geo.Q, geo.C, geo.S, geo.D, geo.X
    R2, RP, Q2 = geo.R2, geo.RP, geo.Q2
    n, wide = R2 * D, Q2 * LANES

    def swap(x):
        y = x.reshape(D, 1, x.shape[0] // D * LANES)
        y = lax.all_to_all(y, ("sub", "fdr"), split_axis=0, concat_axis=0, tiled=True)
        return y.reshape(x.shape)

    slice_index = lax.axis_index("fdr").astype(i32).reshape(1)
    begin, advance = feeder_calls(
        geo, iface_rows.T, substation_of, live_count, inverse, cost, lower_limit, upper_limit
    )
    feeders, base, send = begin()
    state = (
        ((n, wide), f32, VM),
        ((S, wide), f32, VM),
        ((16, LANES), f32, VM),
    )
    out = call(
        functools.partial(owner_first, geo),
        (slice_index, reserve_weight, jnp.swapaxes(reserve_target, 0, 1), swap(send)),
        (SM, SM, VM, VM),
        (
            ((D * 2 * X, LANES), f32, VM),
            ((2 * Q2 * Q2, n, LANES), f32, VM),
            ((R2, RP * S, D), bf16, VM),
            ((RP * n, S), bf16, VM),
            ((n, LANES), f32, VM),
            ((S, wide), f32, VM),
            ((S, LANES), f32, VM),
            ((S, LANES), f32, VM),
        )
        + state,
        (),
        "owner_first",
    )
    send, tables, memory = out[0], out[1:8], out[8:]

    for first in range(2, ITERS - 1, 2):
        feeders, send = advance(feeders, swap(send), False)
        out = call(
            functools.partial(owner_middle, geo, first),
            (swap(send), *tables, *memory),
            (VM,) * 11,
            (((D * 2 * X, LANES), f32, VM),) + state,
            (),
            "owner_middle",
        )
        send, memory = out[0], out[1:]
    setpoints, send = advance(feeders, swap(send), True)
    send, agreed = call(
        functools.partial(owner_last, geo),
        (swap(send), *tables, *memory),
        (VM,) * 11,
        (((D * (X + 1), LANES), f32, VM), ((Q2 * S // RP, LANES), f32, VM)),
        (),
        "owner_last",
    )
    gathered = lax.all_gather(agreed, "fdr", axis=0, tiled=True)
    duals, consensus, norms = call(
        functools.partial(finish, geo),
        (base, swap(send), gathered),
        (SM, VM, VM),
        (((Q, F, C), f32, VM), ((Q, S, C), f32, VM), ((2, ITERS), f32, VM)),
        (pltpu.VMEM((geo.stage_rows, LANES), f32),),
        "finish",
    )
    return jnp.swapaxes(duals, 0, 1), jnp.swapaxes(consensus, 0, 1), norms.T, setpoints


def solution(mesh):
    placed = (
        P(("sub", "fdr"), None, None),
        P(("sub", "fdr"), None, None),
        P(("sub", "fdr"), None),
        P(("sub", "fdr"), None),
        P(("sub", "fdr"), None),
        P(("sub", "fdr")),
        P(("sub", "fdr")),
        P("sub"),
        P("sub", None, None),
    )
    return jax.shard_map(
        functools.partial(shards, mesh.shape["sub"], mesh.shape["fdr"]),
        mesh=mesh,
        in_specs=placed,
        out_specs=(
            P(("sub", "fdr"), None, None),
            P("sub", None, None),
            P(),
            P(("sub", "fdr"), None, None),
        ),
        check_vma=False,
    )
```

```python
import functools

import jax
import jax.numpy as jnp
from jax import lax
from jax.experimental import pallas as pl
from jax.experimental.pallas import tpu as pltpu
from jax.sharding import PartitionSpec as P

ITERS = 5
PENALTY = 2.0
LANES = 128
THIN = 16
GROUP = 8
PIECE = 4

f32 = jnp.float32
bf16 = jnp.bfloat16
i32 = jnp.int32


class Geometry:
    def __init__(self, slots, rows, ifc, scen, owned, n_sub, n_fdr):
        self.F, self.K, self.Q, self.C, self.S = slots, rows, ifc, scen, owned
        self.NB, self.G = n_sub, n_fdr
        self.D = n_sub * n_fdr
        overflow = max(1, slots // (2 * n_sub))
        cap = max(2, slots // n_sub + overflow)
        self.L = scen // n_fdr
        self.RP = n_fdr // 2
        self.R2 = -(-cap // self.RP)
        self.PR = self.R2 * self.RP
        self.Q2 = ifc // 2
        self.X = self.Q2 * self.R2
        self.stage_rows = self.G * self.X * self.NB
        self.id_lane = self.Q2 * self.PR * self.Q

    def off(self, q):
        q2, qp = divmod(q, 2)
        return (qp * self.RP * self.X + q2 * self.R2) * self.NB


def iota(shape, dim):
    return lax.broadcasted_iota(i32, shape, dim)


def group_mask(shape, g, width):
    lane = iota(shape, 1)
    return (lane >= g * width) & (lane < (g + 1) * width)


def roll(x, shift):
    shift = shift % LANES
    return pltpu.roll(x, shift, 1) if shift else x


def pack(geo, stage, send, chunk, off):
    n = geo.X * geo.NB
    for j in range(geo.G):
        acc = None
        for g in range(geo.G):
            v = roll(stage[g * n : (g + 1) * n, :], (g - j) * geo.L)
            acc = v if acc is None else jnp.where(group_mask((n, LANES), g, geo.L), v, acc)
        for x in range(geo.X):
            send[pl.ds(j * chunk + off + x, geo.NB, stride=geo.G * chunk), :] = acc[
                x * geo.NB : (x + 1) * geo.NB
            ]


def unpack(geo, recv, stage, chunk, off):
    n = geo.X * geo.NB
    parts = [
        jnp.concatenate(
            [
                recv[pl.ds(j * chunk + off + x, geo.NB, stride=geo.G * chunk), :]
                for x in range(geo.X)
            ],
            axis=0,
        )
        for j in range(geo.G)
    ]
    for g in range(geo.G):
        acc = None
        for j in range(geo.G):
            v = roll(parts[j], (j - g) * geo.L)
            acc = v if acc is None else jnp.where(group_mask((n, LANES), j, geo.L), v, acc)
        stage[g * n : (g + 1) * n, :] = acc


def dot(a, b):
    return jnp.dot(a, b, preferred_element_type=f32)


def limits(geo, turned, u):
    shape = (geo.K, LANES)
    low = jnp.broadcast_to(turned[:, u : u + 1], shape)
    return low, jnp.broadcast_to(turned[:, geo.F + u : geo.F + u + 1], shape)


def clip(x, low, high):
    return jnp.minimum(jnp.maximum(x, low), high)


def moves(pairs, sems, size):
    def one(i, c):
        src, dst = pairs[i]
        part = pl.ds(c * size, size)
        return pltpu.make_async_copy(src.at[part], dst.at[part], sems.at[i, c])

    return pairs[0][0].shape[0] // size, one


def sweep(slots, body):
    body(0, PIECE)
    body(PIECE, PIECE)

    def step(i, carry):
        body((i + 1) * GROUP, GROUP)
        return carry

    lax.fori_loop(0, slots // GROUP - 1, step, 0)


def pick(work, iface, f, q):
    return work[pl.ds(iface[q, f], 1), :]


def feeder_first(geo, iface, sub, live, inverse, cost, lower, upper,
                 rounded, kept, lim, base, send,
                 inv, price, out, sems, out_sems,
                 stage1, stage2, meta, count, rank, edge, edge_sems, turned, *works):
    F, K, Q, NB, X = geo.F, geo.K, geo.Q, geo.NB, geo.X
    chunk = 2 * X + 2
    bound, square, left, ahead = (works[i * GROUP : (i + 1) * GROUP] for i in range(4))
    pieces, load = moves(((inverse, inv), (cost, price)), sems, PIECE)
    _, store = moves(((out, rounded),), out_sems, PIECE)
    sides = [
        pltpu.make_async_copy(x, edge.at[pl.ds(i * F, F)], edge_sems.at[i])
        for i, x in enumerate((lower, upper))
    ]
    for copy in sides:
        copy.start()
    for c in range(pieces):
        for i in range(2):
            load(i, c).start()
    for k in range(NB):
        count[k] = 0

    def place(f, carry):
        k = lax.div(sub[f], geo.S)
        r = count[k]
        count[k] = r + 1
        rank[f] = r
        base[f] = (lax.rem(r, geo.RP) * X + lax.div(r, geo.RP)) * NB + k
        return carry

    lax.fori_loop(0, F, place, 0)
    edge[2 * F :, :] = jnp.zeros((LANES - 2 * F, K), f32)
    for copy in sides:
        copy.wait()
    lim[...] = edge[...].T
    stage1[...] = jnp.zeros_like(stage1)
    stage2[...] = jnp.zeros_like(stage2)
    meta[...] = jnp.zeros_like(meta)
    kept[...] = jnp.zeros_like(kept)
    lane = iota((1, LANES), 1)
    third = jnp.zeros((1, LANES), i32)
    for i in range(1, geo.Q2 + 1):
        third = third + jnp.where(lane >= i * geo.PR * Q, 1, 0)
    within = lane - third * (geo.PR * Q)

    def body(at, size):
        for c in range(size // PIECE):
            for i in range(2):
                load(i, at // PIECE + c).wait()
        fs = [at + u for u in range(size)]
        turned[...] = pltpu.roll(lim[...], LANES - at, 1)
        for u, f in enumerate(fs):
            near = within - rank[f] * Q
            chosen = jnp.full((1, LANES), -1, i32)
            for q in range(Q):
                chosen = jnp.where((near == q) & (third < geo.Q2), iface[q, f], chosen)
            hot = (iota((K, LANES), 0) == jnp.broadcast_to(chosen, (K, LANES))).astype(f32)
            price_u = price[f]
            both = dot(inv[f], jnp.concatenate([-price_u, hot], axis=1).astype(bf16))
            primal = both[:, :LANES]
            bound[u][...] = primal
            square[u][...] = both[:, LANES:]
            low, high = limits(geo, turned, u)
            t = clip(primal, low, high) - price_u
            left[u][...] = t
            t = t.astype(bf16)
            out[f] = t
            ahead[u][...] = dot(inv[f], t)
            if u % PIECE == PIECE - 1:
                store(0, at // PIECE + u // PIECE).start()
        for u, f in enumerate(fs):
            k = lax.div(sub[f], geo.S)
            ident = jnp.where(f < live[0], sub[f] - k * geo.S + 1, 0).astype(f32)
            lines = [jnp.where(lane == geo.id_lane + rank[f], ident, 0.0),
                     jnp.zeros((1, LANES), f32)]
            to = base[f]
            for q in range(Q):
                m, i = divmod(q, geo.Q2)
                lines[m] = lines[m] + jnp.where(third == i, pick(square[u], iface, f, q), 0.0)
                stage1[pl.ds(to + geo.off(q), 1), :] = pick(bound[u], iface, f, q)
                stage2[pl.ds(to + geo.off(q), 1), :] = pick(ahead[u], iface, f, q)
                kept[f, q : q + 1, :] = pick(left[u], iface, f, q)
            for m in range(2):
                spot = pl.ds(m * NB + k, 1)
                meta[spot, :] = meta[spot, :] + lines[m]

    sweep(F, body)
    pack(geo, stage1, send, chunk, 0)
    pack(geo, stage2, send, chunk, X)
    for j in range(geo.G):
        for m in range(2):
            send[pl.ds(j * chunk + 2 * X + m, NB, stride=geo.G * chunk), :] = meta[
                m * NB : (m + 1) * NB
            ]
    for c in range(pieces):
        store(0, c).wait()


def raise_rows(geo, f, iface, base, rows, work, stage):
    at = base[f]
    rows = [rows[q] + stage[pl.ds(at + geo.off(q), 1), :] for q in range(geo.Q)]
    for q in range(geo.Q):
        work[pl.ds(iface[q, f], 1), :] = rows[q]


def feeder_pair(geo, last, iface, base, live, inverse, cost, rounded, kept, lim, recv, *rest):
    if last:
        result, send, inv, price, held, out, sems, out_sems = rest[:8]
        rest = rest[8:]
    else:
        result, kept_out, send, inv, price, held, out, sems, out_sems = rest[:9]
        rest = rest[9:]
    ways = 1 if last else 2
    arrived, leaving, works = rest[:2], rest[2 : 2 + ways], rest[2 + ways :]
    turned, works = works[0], works[1:]
    side, bound, left, ahead, lows, highs = (works[i * GROUP : (i + 1) * GROUP] for i in range(6))
    pieces, load = moves(((inverse, inv), (cost, price), (rounded, held)), sems, PIECE)
    _, store = moves(((out, result),), out_sems, PIECE)
    for c in range(pieces):
        for i in range(3):
            load(i, c).start()
    for s in range(2):
        unpack(geo, recv, arrived[s], 2 * geo.X, s * geo.X)
    for stage in leaving:
        stage[...] = jnp.zeros_like(stage)
    if not last:
        kept_out[...] = jnp.zeros_like(kept_out)

    def body(at, size):
        for c in range(size // PIECE):
            for i in range(3):
                load(i, at // PIECE + c).wait()
        fs = [at + u for u in range(size)]
        turned[...] = pltpu.roll(lim[...], LANES - at, 1)
        for u, f in enumerate(fs):
            side[u][...] = held[f].astype(f32)
            rows = [kept[f, q : q + 1, :] for q in range(geo.Q)]
            raise_rows(geo, f, iface, base, rows, side[u], arrived[0])
        for u, f in enumerate(fs):
            low, high = limits(geo, turned, u)
            lows[u][...] = low
            highs[u][...] = high
            left[u][...] = clip(dot(inv[f], side[u][...].astype(bf16)), low, high) - price[f]
        for u, f in enumerate(fs):
            rows = [pick(left[u], iface, f, q) for q in range(geo.Q)]
            raise_rows(geo, f, iface, base, rows, left[u], arrived[1])
        for u, f in enumerate(fs):
            low, high = lows[u][...], highs[u][...]
            primal = dot(inv[f], left[u][...].astype(bf16))
            bound[u][...] = primal
            anchor = clip(primal, low, high)
            if last:
                out[f] = anchor * jnp.where(f < live[0], 1.0, 0.0)
            else:
                t = anchor - price[f]
                side[u][...] = t
                t = t.astype(bf16)
                out[f] = t
                ahead[u][...] = dot(inv[f], t)
            if u % PIECE == PIECE - 1:
                store(0, at // PIECE + u // PIECE).start()
        for u, f in enumerate(fs):
            to = base[f]
            for q in range(geo.Q):
                leaving[0][pl.ds(to + geo.off(q), 1), :] = pick(bound[u], iface, f, q)
                if not last:
                    leaving[1][pl.ds(to + geo.off(q), 1), :] = pick(ahead[u], iface, f, q)
                    kept_out[f, q : q + 1, :] = pick(side[u], iface, f, q)

    sweep(geo.F, body)
    for s in range(ways):
        pack(geo, leaving[s], send, ways * geo.X, s * geo.X)
    for c in range(pieces):
        store(0, c).wait()


def slice_parity(geo, shape):
    lane = iota(shape, 1)
    half = geo.RP * geo.L
    qp = jnp.where(lane >= half, 1, 0)
    inner = lane - qp * half
    rp = jnp.zeros(shape, i32)
    for i in range(1, geo.RP):
        rp = rp + jnp.where(inner >= i * geo.L, 1, 0)
    return qp, rp


def owner_setup(geo, slice_index, weight, aim, recv, coef, hot_t, hot, act, scaled, den, count):
    X, D, S, Q, Q2, R2, RP, PR = geo.X, geo.D, geo.S, geo.Q, geo.Q2, geo.R2, geo.RP, geo.PR
    chunk = 2 * X + 2
    metas = [recv[pl.ds(2 * X + m, D, stride=chunk), :] for m in range(2)]
    qp, rp = slice_parity(geo, (D, LANES))
    padded = metas[0]
    if D < LANES:
        padded = jnp.concatenate([padded, jnp.zeros((LANES - D, LANES), f32)], axis=0)
    turned = padded.T
    total = jnp.zeros((S, D), f32)
    for r2 in range(R2):
        live = jnp.zeros((D, LANES), f32)
        for p in range(RP):
            r = r2 * RP + p
            col = metas[0][:, geo.id_lane + r : geo.id_lane + r + 1]
            wide = jnp.broadcast_to(col, (D, LANES))
            live = jnp.where(rp == p, jnp.where(wide > 0.5, 1.0, 0.0), live)
            mine = (wide == (iota((D, LANES), 1) + 1).astype(f32)).astype(f32)
            hot[(p * R2 + r2) * D : (p * R2 + r2 + 1) * D, :] = mine[:, :S].astype(bf16)
            row = turned[geo.id_lane + r : geo.id_lane + r + 1, :D]
            theirs = (
                jnp.broadcast_to(row, (S, D)) == (iota((S, D), 0) + 1).astype(f32)
            ).astype(f32)
            total = total + theirs
            hot_t[r2, p * S : (p + 1) * S, :] = theirs.astype(bf16)
        act[r2 * D : (r2 + 1) * D, :] = live
    members = jnp.sum(total, axis=1, keepdims=True)
    w = jnp.zeros((S, LANES), f32)
    for s in range(S):
        w = jnp.where(iota((S, LANES), 0) == s, weight[s], w)
    members = jnp.broadcast_to(members, (S, LANES))
    den[...] = members + w
    qps, rps = slice_parity(geo, (S, LANES))
    count[...] = jnp.where(rps == 0, members, 0.0)
    lane = iota((S, LANES), 1)
    inner = lane - (qps * RP + rps) * geo.L
    index = inner + slice_index * geo.L
    for q2 in range(Q2):
        even = jnp.take_along_axis(aim[2 * q2], index, axis=1)
        odd = jnp.take_along_axis(aim[2 * q2 + 1], index, axis=1)
        scaled[:, q2 * LANES : (q2 + 1) * LANES] = w * jnp.where(qps == 0, even, odd)
    for par in range(2):
        for q2 in range(Q2):
            for q2p in range(Q2):
                for r2 in range(R2):
                    sides = []
                    for side in range(2):
                        q = 2 * q2 + side
                        other = 2 * q2p + (side if par == 0 else 1 - side)
                        sides.append((q // Q2, (q % Q2) * PR * Q + r2 * RP * Q + other))
                    idx = rp * Q + jnp.where(qp == 0, sides[0][1], sides[1][1])
                    if sides[0][0] == sides[1][0]:
                        value = jnp.take_along_axis(metas[sides[0][0]], idx, axis=1)
                    else:
                        value = jnp.where(
                            qp == 0,
                            jnp.take_along_axis(metas[sides[0][0]], idx, axis=1),
                            jnp.take_along_axis(metas[sides[1][0]], idx, axis=1),
                        )
                    coef[(par * Q2 + q2) * Q2 + q2p, r2 * D : (r2 + 1) * D, :] = value


def arrive(geo, recv, chunk, off):
    return [
        jnp.concatenate(
            [
                recv[pl.ds(off + q2 * geo.R2 + r2, geo.D, stride=chunk), :]
                for r2 in range(geo.R2)
            ],
            axis=0,
        )
        for q2 in range(geo.Q2)
    ]


def depart(geo, values, send, chunk, off):
    for q2 in range(geo.Q2):
        for r2 in range(geo.R2):
            send[pl.ds(off + q2 * geo.R2 + r2, geo.D, stride=chunk), :] = values[q2][
                r2 * geo.D : (r2 + 1) * geo.D
            ]


def split(x):
    high = x.astype(bf16)
    return high, (x - high.astype(f32)).astype(bf16)


def owner_step(geo, h, raised, dual, old, coef, hot_t, hot, act, scaled, den, count):
    D, S, Q2, R2, RP = geo.D, geo.S, geo.Q2, geo.R2, geo.RP
    n = R2 * D
    rows = list(h)
    if raised is not None:
        turned = [roll(v, geo.RP * geo.L) for v in raised]
        for q2 in range(Q2):
            acc = rows[q2]
            for q2p in range(Q2):
                acc = acc + coef[q2 * Q2 + q2p] * raised[q2p]
                acc = acc + coef[(Q2 + q2) * Q2 + q2p] * turned[q2p]
            rows[q2] = acc
    if dual is not None:
        rows = [b + u for b, u in zip(rows, dual)]
    high, low = split(jnp.concatenate(rows, axis=1))
    sums = None
    for r2 in range(R2):
        part = slice(r2 * D, (r2 + 1) * D)
        term = dot(hot_t[r2], high[part]) + dot(hot_t[r2], low[part])
        sums = term if sums is None else sums + term
    _, rps = slice_parity(geo, (S, LANES))
    fresh = []
    for q2 in range(Q2):
        cols = slice(q2 * LANES, (q2 + 1) * LANES)
        mine = sums[0:S, cols]
        for p in range(1, RP):
            mine = jnp.where(rps == p, sums[p * S : (p + 1) * S, cols], mine)
        whole = mine
        for s in range(1, RP):
            whole = whole + jnp.where(rps >= s, roll(mine, s * geo.L), 0.0)
            whole = whole + jnp.where(rps < RP - s, roll(mine, -s * geo.L), 0.0)
        fresh.append((whole + scaled[:, cols]) / den[...])
    high, low = split(jnp.concatenate(fresh, axis=1))
    back = dot(hot[...], high) + dot(hot[...], low)
    _, rpn = slice_parity(geo, (n, LANES))
    new_dual, new_raise = [], []
    moved = jnp.zeros((1, LANES), f32)
    for q2 in range(Q2):
        cols = slice(q2 * LANES, (q2 + 1) * LANES)
        own = back[0:n, cols]
        for p in range(1, RP):
            own = jnp.where(rpn == p, back[p * n : (p + 1) * n, cols], own)
        u = (rows[q2] - own) * act[...]
        new_dual.append(u)
        new_raise.append(PENALTY * (own - u))
        step = u if dual is None else u - dual[q2]
        moved = moved + jnp.sum(step * step, axis=0, keepdims=True)
    shifted = jnp.zeros((1, LANES), f32)
    for q2 in range(Q2):
        gap = fresh[q2] if old is None else fresh[q2] - old[q2]
        shifted = shifted + jnp.sum(count[...] * gap * gap, axis=0, keepdims=True)
    return new_dual, new_raise, fresh, moved, shifted


def read_list(geo, ref):
    return [ref[:, q2 * LANES : (q2 + 1) * LANES] for q2 in range(geo.Q2)]


def write_list(geo, ref, values):
    for q2 in range(geo.Q2):
        ref[:, q2 * LANES : (q2 + 1) * LANES] = values[q2]


def owner_first(geo, slice_index, weight, aim, recv,
                send, coef, hot_t, hot, act, scaled, den, count, dual, old, norms):
    X = geo.X
    owner_setup(geo, slice_index[0], weight, aim, recv, coef, hot_t, hot, act, scaled, den, count)
    tables = (coef, hot_t, hot, act, scaled, den, count)
    chunk = 2 * X + 2
    h = arrive(geo, recv, chunk, 0)
    u, v, z, p0, d0 = owner_step(geo, h, None, None, None, *tables)
    depart(geo, v, send, 2 * X, 0)
    h = arrive(geo, recv, chunk, X)
    u, v, z, p1, d1 = owner_step(geo, h, v, u, z, *tables)
    depart(geo, v, send, 2 * X, X)
    write_list(geo, dual, u)
    write_list(geo, old, z)
    norms[...] = jnp.zeros_like(norms)
    for i, value in enumerate((p0, d0, p1, d1)):
        norms[i : i + 1] = value


def owner_middle(geo, first, recv, coef, hot_t, hot, act, scaled, den, count,
                 dual, old, norms, send, dual_out, old_out, norms_out):
    X = geo.X
    tables = (coef, hot_t, hot, act, scaled, den, count)
    u, v, z = read_list(geo, dual), None, read_list(geo, old)
    norms_out[...] = norms[...]
    for s in range(2):
        h = arrive(geo, recv, 2 * X, s * X)
        u, v, z, p, d = owner_step(geo, h, v if s else None, u, z, *tables)
        depart(geo, v, send, 2 * X, s * X)
        at = 2 * (first + s)
        norms_out[at : at + 1] = p
        norms_out[at + 1 : at + 2] = d
    write_list(geo, dual_out, u)
    write_list(geo, old_out, z)


def owner_last(geo, recv, coef, hot_t, hot, act, scaled, den, count,
               dual, old, norms, send, agreed):
    X, S, RP = geo.X, geo.S, geo.RP
    tables = (coef, hot_t, hot, act, scaled, den, count)
    u, v, z = read_list(geo, dual), None, read_list(geo, old)
    h = arrive(geo, recv, X, 0)
    u, v, z, p, d = owner_step(geo, h, None, u, z, *tables)
    depart(geo, [PENALTY * x for x in u], send, X + 1, 0)
    at = 2 * (ITERS - 1)
    everything = norms[...]
    rows = everything.shape[0]
    row = iota((rows, LANES), 0)
    everything = jnp.where(row == at, p, everything)
    everything = jnp.where(row == at + 1, d, everything)
    sums = jnp.sum(everything, axis=1, keepdims=True)
    line = jnp.sum(jnp.where(row == iota((rows, LANES), 1), sums, 0.0), axis=0, keepdims=True)
    send[pl.ds(X, geo.D, stride=X + 1), :] = jnp.broadcast_to(line, (geo.D, LANES))
    part = S // RP
    _, rps = slice_parity(geo, (part, LANES))
    for q2 in range(geo.Q2):
        value = z[q2][0:part]
        for i in range(1, RP):
            value = jnp.where(rps == i, z[q2][i * part : (i + 1) * part], value)
        agreed[q2 * part : (q2 + 1) * part, :] = value


def finish(geo, base, recv, agreed, duals, consensus, norms, stage):
    X, S, RP, G, L = geo.X, geo.S, geo.RP, geo.G, geo.L
    unpack(geo, recv, stage, X + 1, 0)

    def body(f, carry):
        at = base[f]
        for q in range(geo.Q):
            duals[q, pl.ds(f, 1), :] = stage[pl.ds(at + geo.off(q), 1), :]
        return carry

    lax.fori_loop(0, geo.F, body, 0)
    part = S // RP
    n = geo.Q2 * part
    for q2 in range(geo.Q2):
        sides = [agreed[j * n + q2 * part : j * n + (q2 + 1) * part, :] for j in range(G)]
        for qp in range(2):
            for rp in range(RP):
                acc = None
                for j in range(G):
                    v = roll(sides[j], (j - (qp * RP + rp)) * L)
                    acc = v if acc is None else jnp.where(group_mask((part, LANES), j, L), v, acc)
                consensus[2 * q2 + qp, rp * part : (rp + 1) * part, :] = acc
    line = jnp.sum(recv[pl.ds(X, geo.D, stride=X + 1), :], axis=0, keepdims=True)
    line = jnp.broadcast_to(jnp.sqrt(line), (8, LANES))
    side = iota((8, LANES), 0)
    lane = iota((8, LANES), 1)
    table = jnp.zeros((8, LANES), f32)
    for i in range(ITERS):
        table = jnp.where((lane == i) & (side == 0), roll(line, -i), table)
        table = jnp.where((lane == i) & (side == 1), PENALTY * roll(line, -i - 1), table)
    norms[...] = table[:2, :ITERS]


VM = pltpu.VMEM
SM = pltpu.SMEM
HB = pltpu.HBM
SMH = 0


def call(body, args, ins, outs, scratch=(), name=None):
    args = [
        pltpu.with_memory_space_constraint(x, HB) if s in (HB, SMH) else x
        for x, s in zip(args, ins)
    ]
    ins = [SM if s is SMH else s for s in ins]
    return pl.pallas_call(
        body,
        in_specs=[pl.BlockSpec(memory_space=s) for s in ins],
        out_specs=[pl.BlockSpec(memory_space=s) for _, _, s in outs],
        out_shape=[
            jax.ShapeDtypeStruct(shape, dtype) if s is VM else s(shape, dtype)
            for shape, dtype, s in outs
        ],
        scratch_shapes=list(scratch),
        compiler_params=pltpu.CompilerParams(vmem_limit_bytes=40 << 20),
        name=name,
    )(*args)


def feeder_calls(geo, iface, substation_of, live_count, inverse, cost, lower, upper):
    F, K, C, D, X = geo.F, geo.K, geo.C, geo.D, geo.X
    pieces = F // PIECE
    stage = pltpu.VMEM((geo.stage_rows, LANES), f32)
    works = (pltpu.VMEM((K, LANES), f32),) * (4 * GROUP)
    squares = pltpu.VMEM((F, K, K), bf16)
    prices = pltpu.VMEM((F, K, C), f32)
    halves = pltpu.VMEM((F, K, C), bf16)
    carried = (((F, K, C), bf16, HB), ((F, 8, C), f32, VM))

    def sems(count):
        return pltpu.SemaphoreType.DMA((count, pieces))

    def begin():
        rounded, kept, lim, base, send = call(
            functools.partial(feeder_first, geo),
            (iface, substation_of, live_count, inverse, cost, lower, upper),
            (SMH, SMH, SM, HB, HB, HB, HB),
            carried
            + (
                ((K, LANES), f32, VM),
                ((F,), i32, SM),
                ((D * (2 * X + 2), LANES), f32, VM),
            ),
            (squares, prices, halves, sems(2), sems(1),
             stage, stage, pltpu.VMEM((2 * geo.NB, LANES), f32), pltpu.SMEM((geo.NB,), i32),
             pltpu.SMEM((F,), i32), pltpu.VMEM((LANES, K), f32),
             pltpu.SemaphoreType.DMA((2,)), pltpu.VMEM((K, LANES), f32)) + works,
            "feeder_first",
        )
        return (rounded, kept, lim, base), base, send

    def advance(state, recv, last):
        rounded, kept, lim, base = state
        out = call(
            functools.partial(feeder_pair, geo, last),
            (iface, base, live_count, inverse, cost, rounded, kept, lim, recv),
            (SM, SM, SM, HB, HB, HB, VM, VM, VM),
            ((((F, K, C), f32, HB),) if last else carried)
            + (((D * (1 if last else 2) * X, LANES), f32, VM),),
            (squares, prices, halves, prices if last else halves, sems(3), sems(1))
            + (stage,) * (3 if last else 4) + (pltpu.VMEM((K, LANES), f32),) + works + works[: 2 * GROUP],
            "feeder_last" if last else "feeder_pair",
        )
        return out if last else ((out[0], out[1], lim, base), out[2])

    return begin, advance


def shards(
    n_sub,
    n_fdr,
    inverse,
    cost,
    lower_limit,
    upper_limit,
    iface_rows,
    substation_of,
    live_count,
    reserve_weight,
    reserve_target,
):
    slots, rows, scen = cost.shape
    geo = Geometry(slots, rows, iface_rows.shape[1], scen, reserve_weight.shape[0], n_sub, n_fdr)
    F, K, Q, C, S, D, X = geo.F, geo.K, geo.Q, geo.C, geo.S, geo.D, geo.X
    R2, RP, Q2 = geo.R2, geo.RP, geo.Q2
    n, wide = R2 * D, Q2 * LANES

    def swap(x):
        y = x.reshape(D, 1, x.shape[0] // D * LANES)
        y = lax.all_to_all(y, ("sub", "fdr"), split_axis=0, concat_axis=0, tiled=True)
        return y.reshape(x.shape)

    slice_index = lax.axis_index("fdr").astype(i32).reshape(1)
    begin, advance = feeder_calls(
        geo, iface_rows.T, substation_of, live_count, inverse, cost, lower_limit, upper_limit
    )
    feeders, base, send = begin()
    state = (
        ((n, wide), f32, VM),
        ((S, wide), f32, VM),
        ((16, LANES), f32, VM),
    )
    out = call(
        functools.partial(owner_first, geo),
        (slice_index, reserve_weight, jnp.swapaxes(reserve_target, 0, 1), swap(send)),
        (SM, SM, VM, VM),
        (
            ((D * 2 * X, LANES), f32, VM),
            ((2 * Q2 * Q2, n, LANES), f32, VM),
            ((R2, RP * S, D), bf16, VM),
            ((RP * n, S), bf16, VM),
            ((n, LANES), f32, VM),
            ((S, wide), f32, VM),
            ((S, LANES), f32, VM),
            ((S, LANES), f32, VM),
        )
        + state,
        (),
        "owner_first",
    )
    send, tables, memory = out[0], out[1:8], out[8:]

    for first in range(2, ITERS - 1, 2):
        feeders, send = advance(feeders, swap(send), False)
        out = call(
            functools.partial(owner_middle, geo, first),
            (swap(send), *tables, *memory),
            (VM,) * 11,
            (((D * 2 * X, LANES), f32, VM),) + state,
            (),
            "owner_middle",
        )
        send, memory = out[0], out[1:]
    setpoints, send = advance(feeders, swap(send), True)
    send, agreed = call(
        functools.partial(owner_last, geo),
        (swap(send), *tables, *memory),
        (VM,) * 11,
        (((D * (X + 1), LANES), f32, VM), ((Q2 * S // RP, LANES), f32, VM)),
        (),
        "owner_last",
    )
    gathered = lax.all_gather(agreed, "fdr", axis=0, tiled=True)
    duals, consensus, norms = call(
        functools.partial(finish, geo),
        (base, swap(send), gathered),
        (SM, VM, VM),
        (((Q, F, C), f32, VM), ((Q, S, C), f32, VM), ((2, ITERS), f32, VM)),
        (pltpu.VMEM((geo.stage_rows, LANES), f32),),
        "finish",
    )
    return jnp.swapaxes(duals, 0, 1), jnp.swapaxes(consensus, 0, 1), norms.T, setpoints


def solution(mesh):
    placed = (
        P(("sub", "fdr"), None, None),
        P(("sub", "fdr"), None, None),
        P(("sub", "fdr"), None),
        P(("sub", "fdr"), None),
        P(("sub", "fdr"), None),
        P(("sub", "fdr")),
        P(("sub", "fdr")),
        P("sub"),
        P("sub", None, None),
    )
    return jax.shard_map(
        functools.partial(shards, mesh.shape["sub"], mesh.shape["fdr"]),
        mesh=mesh,
        in_specs=placed,
        out_specs=(
            P(("sub", "fdr"), None, None),
            P("sub", None, None),
            P(),
            P(("sub", "fdr"), None, None),
        ),
        check_vma=False,
    )
```

```python
import functools

import jax
import jax.numpy as jnp
from jax import lax
from jax.experimental import pallas as pl
from jax.experimental.pallas import tpu as pltpu
from jax.sharding import PartitionSpec as P

ITERS = 5
PENALTY = 2.0
LANES = 128
THIN = 16
GROUP = 8
PIECE = 4

f32 = jnp.float32
bf16 = jnp.bfloat16
i32 = jnp.int32


class Geometry:
    def __init__(self, slots, rows, ifc, scen, owned, n_sub, n_fdr):
        self.F, self.K, self.Q, self.C, self.S = slots, rows, ifc, scen, owned
        self.NB, self.G = n_sub, n_fdr
        self.D = n_sub * n_fdr
        overflow = max(1, slots // (2 * n_sub))
        cap = max(2, slots // n_sub + overflow)
        self.L = scen // n_fdr
        self.RP = n_fdr // 2
        self.R2 = -(-cap // self.RP)
        self.PR = self.R2 * self.RP
        self.Q2 = ifc // 2
        self.X = self.Q2 * self.R2
        self.stage_rows = self.G * self.X * self.NB
        self.id_lane = self.Q2 * self.PR * self.Q

    def off(self, q):
        q2, qp = divmod(q, 2)
        return (qp * self.RP * self.X + q2 * self.R2) * self.NB


def iota(shape, dim):
    return lax.broadcasted_iota(i32, shape, dim)


def group_mask(shape, g, width):
    lane = iota(shape, 1)
    return (lane >= g * width) & (lane < (g + 1) * width)


def roll(x, shift):
    shift = shift % LANES
    return pltpu.roll(x, shift, 1) if shift else x


def pack(geo, stage, send, chunk, off):
    n = geo.X * geo.NB
    for j in range(geo.G):
        acc = None
        for g in range(geo.G):
            v = roll(stage[g * n : (g + 1) * n, :], (g - j) * geo.L)
            acc = v if acc is None else jnp.where(group_mask((n, LANES), g, geo.L), v, acc)
        for x in range(geo.X):
            send[pl.ds(j * chunk + off + x, geo.NB, stride=geo.G * chunk), :] = acc[
                x * geo.NB : (x + 1) * geo.NB
            ]


def unpack(geo, recv, stage, chunk, off):
    n = geo.X * geo.NB
    parts = [
        jnp.concatenate(
            [
                recv[pl.ds(j * chunk + off + x, geo.NB, stride=geo.G * chunk), :]
                for x in range(geo.X)
            ],
            axis=0,
        )
        for j in range(geo.G)
    ]
    for g in range(geo.G):
        acc = None
        for j in range(geo.G):
            v = roll(parts[j], (j - g) * geo.L)
            acc = v if acc is None else jnp.where(group_mask((n, LANES), j, geo.L), v, acc)
        stage[g * n : (g + 1) * n, :] = acc


def dot(a, b):
    return jnp.dot(a, b, preferred_element_type=f32)


def limits(geo, turned, u):
    shape = (geo.K, LANES)
    low = jnp.broadcast_to(turned[:, u : u + 1], shape)
    return low, jnp.broadcast_to(turned[:, geo.F + u : geo.F + u + 1], shape)


def clip(x, low, high):
    return jnp.minimum(jnp.maximum(x, low), high)


def moves(pairs, sems, size):
    def one(i, c):
        src, dst = pairs[i]
        part = pl.ds(c * size, size)
        return pltpu.make_async_copy(src.at[part], dst.at[part], sems.at[i, c])

    return pairs[0][0].shape[0] // size, one


def sweep(slots, body):
    def step(i, carry):
        body(i * GROUP, GROUP)
        return carry

    lax.fori_loop(0, slots // GROUP, step, 0)


def pick(work, iface, f, q):
    return work[pl.ds(iface[q, f], 1), :]


def feeder_first(geo, rows_in, sub_in, live, slice_index, inverse, cost, lower, upper,
                 rounded, kept, lim, base, iface, send,
                 inv, price, out, sems, out_sems,
                 stage1, stage2, meta, count, rank, sub, edge, edge_sems, turned, *works):
    F, K, Q, NB, X = geo.F, geo.K, geo.Q, geo.NB, geo.X
    chunk = 2 * X + 2
    bound, square, left, ahead = (works[i * GROUP : (i + 1) * GROUP] for i in range(4))
    pieces, load = moves(((inverse, inv), (cost, price)), sems, PIECE)
    _, store = moves(((out, rounded),), out_sems, PIECE)
    sides = [
        pltpu.make_async_copy(x, edge.at[pl.ds(i * F, F)], edge_sems.at[i])
        for i, x in enumerate((lower, upper))
    ]
    tables = [
        pltpu.make_async_copy(x, y, edge_sems.at[2 + i])
        for i, (x, y) in enumerate(((sub_in, sub), (rows_in, iface)))
    ]
    for copy in tables + sides:
        copy.start()
    for c in range(pieces):
        for i in range(2):
            load(i, c).start()
    for copy in tables:
        copy.wait()
    for k in range(NB):
        count[k] = 0

    def place(f, carry):
        k = lax.div(sub[f], geo.S)
        r = count[k]
        count[k] = r + 1
        rank[f] = r
        base[f] = (lax.rem(r, geo.RP) * X + lax.div(r, geo.RP)) * NB + k
        return carry

    lax.fori_loop(0, F, place, 0)
    edge[2 * F :, :] = jnp.zeros((LANES - 2 * F, K), f32)
    for copy in sides:
        copy.wait()
    lim[...] = edge[...].T
    stage1[...] = jnp.zeros_like(stage1)
    stage2[...] = jnp.zeros_like(stage2)
    meta[...] = jnp.zeros_like(meta)
    kept[...] = jnp.zeros_like(kept)
    lane = iota((1, LANES), 1)
    third = jnp.zeros((1, LANES), i32)
    for i in range(1, geo.Q2 + 1):
        third = third + jnp.where(lane >= i * geo.PR * Q, 1, 0)
    within = lane - third * (geo.PR * Q)

    def body(at, size):
        for c in range(size // PIECE):
            for i in range(2):
                load(i, at // PIECE + c).wait()
        fs = [at + u for u in range(size)]
        turned[...] = pltpu.roll(lim[...], LANES - at, 1)
        for u, f in enumerate(fs):
            near = within - rank[f] * Q
            chosen = jnp.full((1, LANES), -1, i32)
            for q in range(Q):
                chosen = jnp.where((near == q) & (third < geo.Q2), iface[q, f], chosen)
            hot = (iota((K, LANES), 0) == jnp.broadcast_to(chosen, (K, LANES))).astype(f32)
            price_u = price[f]
            both = dot(inv[f], jnp.concatenate([-price_u, hot], axis=1).astype(bf16))
            primal = both[:, :LANES]
            bound[u][...] = primal
            square[u][...] = both[:, LANES:]
            low, high = limits(geo, turned, u)
            t = clip(primal, low, high) - price_u
            left[u][...] = t
            t = t.astype(bf16)
            out[f] = t
            ahead[u][...] = dot(inv[f], t)
            if u % PIECE == PIECE - 1:
                store(0, at // PIECE + u // PIECE).start()
        for u, f in enumerate(fs):
            k = lax.div(sub[f], geo.S)
            ident = jnp.where(f < live[0], sub[f] - k * geo.S + 1, 0).astype(f32)
            lines = [jnp.where(lane == geo.id_lane + rank[f], ident, 0.0),
                     jnp.zeros((1, LANES), f32)]
            to = base[f]
            for q in range(Q):
                m, i = divmod(q, geo.Q2)
                lines[m] = lines[m] + jnp.where(third == i, pick(square[u], iface, f, q), 0.0)
                stage1[pl.ds(to + geo.off(q), 1), :] = pick(bound[u], iface, f, q)
                stage2[pl.ds(to + geo.off(q), 1), :] = pick(ahead[u], iface, f, q)
                kept[f, q : q + 1, :] = pick(left[u], iface, f, q)
            for m in range(2):
                spot = pl.ds(m * NB + k, 1)
                meta[spot, :] = meta[spot, :] + lines[m]

    sweep(F, body)
    pack(geo, stage1, send, chunk, 0)
    pack(geo, stage2, send, chunk, X)
    for j in range(geo.G):
        for m in range(2):
            send[pl.ds(j * chunk + 2 * X + m, NB, stride=geo.G * chunk), :] = meta[
                m * NB : (m + 1) * NB
            ]
    for c in range(pieces):
        store(0, c).wait()


def raise_rows(geo, f, iface, base, rows, work, stage):
    at = base[f]
    rows = [rows[q] + stage[pl.ds(at + geo.off(q), 1), :] for q in range(geo.Q)]
    for q in range(geo.Q):
        work[pl.ds(iface[q, f], 1), :] = rows[q]


def feeder_pair(geo, last, iface, base, live, inverse, cost, rounded, kept, lim, recv, *rest):
    if last:
        result, send, inv, price, held, out, sems, out_sems = rest[:8]
        rest = rest[8:]
    else:
        result, kept_out, send, inv, price, held, out, sems, out_sems = rest[:9]
        rest = rest[9:]
    ways = 1 if last else 2
    arrived, leaving, works = rest[:2], rest[2 : 2 + ways], rest[2 + ways :]
    turned, works = works[0], works[1:]
    side, bound, left, ahead, lows, highs = (works[i * GROUP : (i + 1) * GROUP] for i in range(6))
    pieces, load = moves(((inverse, inv), (cost, price), (rounded, held)), sems, PIECE)
    _, store = moves(((out, result),), out_sems, PIECE)
    for c in range(pieces):
        for i in range(3):
            load(i, c).start()
    for s in range(2):
        unpack(geo, recv, arrived[s], 2 * geo.X, s * geo.X)
    for stage in leaving:
        stage[...] = jnp.zeros_like(stage)
    if not last:
        kept_out[...] = jnp.zeros_like(kept_out)

    def body(at, size):
        for c in range(size // PIECE):
            for i in range(3):
                load(i, at // PIECE + c).wait()
        fs = [at + u for u in range(size)]
        turned[...] = pltpu.roll(lim[...], LANES - at, 1)
        for u, f in enumerate(fs):
            side[u][...] = held[f].astype(f32)
            rows = [kept[f, q : q + 1, :] for q in range(geo.Q)]
            raise_rows(geo, f, iface, base, rows, side[u], arrived[0])
        for u, f in enumerate(fs):
            low, high = limits(geo, turned, u)
            lows[u][...] = low
            highs[u][...] = high
            left[u][...] = clip(dot(inv[f], side[u][...].astype(bf16)), low, high) - price[f]
        for u, f in enumerate(fs):
            rows = [pick(left[u], iface, f, q) for q in range(geo.Q)]
            raise_rows(geo, f, iface, base, rows, left[u], arrived[1])
        for u, f in enumerate(fs):
            low, high = lows[u][...], highs[u][...]
            primal = dot(inv[f], left[u][...].astype(bf16))
            bound[u][...] = primal
            anchor = clip(primal, low, high)
            if last:
                out[f] = anchor * jnp.where(f < live[0], 1.0, 0.0)
            else:
                t = anchor - price[f]
                side[u][...] = t
                t = t.astype(bf16)
                out[f] = t
                ahead[u][...] = dot(inv[f], t)
            if u % PIECE == PIECE - 1:
                store(0, at // PIECE + u // PIECE).start()
        for u, f in enumerate(fs):
            to = base[f]
            for q in range(geo.Q):
                leaving[0][pl.ds(to + geo.off(q), 1), :] = pick(bound[u], iface, f, q)
                if not last:
                    leaving[1][pl.ds(to + geo.off(q), 1), :] = pick(ahead[u], iface, f, q)
                    kept_out[f, q : q + 1, :] = pick(side[u], iface, f, q)

    sweep(geo.F, body)
    for s in range(ways):
        pack(geo, leaving[s], send, ways * geo.X, s * geo.X)
    for c in range(pieces):
        store(0, c).wait()


def slice_parity(geo, shape):
    lane = iota(shape, 1)
    half = geo.RP * geo.L
    qp = jnp.where(lane >= half, 1, 0)
    inner = lane - qp * half
    rp = jnp.zeros(shape, i32)
    for i in range(1, geo.RP):
        rp = rp + jnp.where(inner >= i * geo.L, 1, 0)
    return qp, rp


def owner_setup(
    geo, slice_index, weight, aim, copies, recv, coef, hot_t, hot, act, scaled, den, count
):
    X, D, S, Q, Q2, R2, RP, PR = geo.X, geo.D, geo.S, geo.Q, geo.Q2, geo.R2, geo.RP, geo.PR
    chunk = 2 * X + 2
    metas = [recv[pl.ds(2 * X + m, D, stride=chunk), :] for m in range(2)]
    qp, rp = slice_parity(geo, (D, LANES))
    padded = metas[0]
    if D < LANES:
        padded = jnp.concatenate([padded, jnp.zeros((LANES - D, LANES), f32)], axis=0)
    turned = padded.T
    total = jnp.zeros((S, D), f32)
    for r2 in range(R2):
        live = jnp.zeros((D, LANES), f32)
        for p in range(RP):
            r = r2 * RP + p
            col = metas[0][:, geo.id_lane + r : geo.id_lane + r + 1]
            wide = jnp.broadcast_to(col, (D, LANES))
            live = jnp.where(rp == p, jnp.where(wide > 0.5, 1.0, 0.0), live)
            mine = (wide == (iota((D, LANES), 1) + 1).astype(f32)).astype(f32)
            hot[(p * R2 + r2) * D : (p * R2 + r2 + 1) * D, :] = mine[:, :S].astype(bf16)
            row = turned[geo.id_lane + r : geo.id_lane + r + 1, :D]
            theirs = (
                jnp.broadcast_to(row, (S, D)) == (iota((S, D), 0) + 1).astype(f32)
            ).astype(f32)
            total = total + theirs
            hot_t[r2, p * S : (p + 1) * S, :] = theirs.astype(bf16)
        act[r2 * D : (r2 + 1) * D, :] = live
    for par in range(2):
        for q2 in range(Q2):
            for q2p in range(Q2):
                for r2 in range(R2):
                    sides = []
                    for side in range(2):
                        q = 2 * q2 + side
                        other = 2 * q2p + (side if par == 0 else 1 - side)
                        sides.append((q // Q2, (q % Q2) * PR * Q + r2 * RP * Q + other))
                    idx = rp * Q + jnp.where(qp == 0, sides[0][1], sides[1][1])
                    if sides[0][0] == sides[1][0]:
                        value = jnp.take_along_axis(metas[sides[0][0]], idx, axis=1)
                    else:
                        value = jnp.where(
                            qp == 0,
                            jnp.take_along_axis(metas[sides[0][0]], idx, axis=1),
                            jnp.take_along_axis(metas[sides[1][0]], idx, axis=1),
                        )
                    coef[(par * Q2 + q2) * Q2 + q2p, r2 * D : (r2 + 1) * D, :] = value
    for copy in copies:
        copy.wait()
    members = jnp.sum(total, axis=1, keepdims=True)
    w = jnp.zeros((S, LANES), f32)
    for s in range(S):
        w = jnp.where(iota((S, LANES), 0) == s, weight[s], w)
    members = jnp.broadcast_to(members, (S, LANES))
    den[...] = members + w
    qps, rps = slice_parity(geo, (S, LANES))
    count[...] = jnp.where(rps == 0, members, 0.0)
    lane = iota((S, LANES), 1)
    inner = lane - (qps * RP + rps) * geo.L
    index = inner + slice_index * geo.L
    for q2 in range(Q2):
        even = jnp.take_along_axis(aim[2 * q2], index, axis=1)
        odd = jnp.take_along_axis(aim[2 * q2 + 1], index, axis=1)
        scaled[:, q2 * LANES : (q2 + 1) * LANES] = w * jnp.where(qps == 0, even, odd)


def arrive(geo, recv, chunk, off):
    return [
        jnp.concatenate(
            [
                recv[pl.ds(off + q2 * geo.R2 + r2, geo.D, stride=chunk), :]
                for r2 in range(geo.R2)
            ],
            axis=0,
        )
        for q2 in range(geo.Q2)
    ]


def depart(geo, values, send, chunk, off):
    for q2 in range(geo.Q2):
        for r2 in range(geo.R2):
            send[pl.ds(off + q2 * geo.R2 + r2, geo.D, stride=chunk), :] = values[q2][
                r2 * geo.D : (r2 + 1) * geo.D
            ]


def split(x):
    high = x.astype(bf16)
    return high, (x - high.astype(f32)).astype(bf16)


def owner_step(geo, h, raised, dual, old, coef, hot_t, hot, act, scaled, den, count):
    D, S, Q2, R2, RP = geo.D, geo.S, geo.Q2, geo.R2, geo.RP
    n = R2 * D
    rows = list(h)
    if raised is not None:
        turned = [roll(v, geo.RP * geo.L) for v in raised]
        for q2 in range(Q2):
            acc = rows[q2]
            for q2p in range(Q2):
                acc = acc + coef[q2 * Q2 + q2p] * raised[q2p]
                acc = acc + coef[(Q2 + q2) * Q2 + q2p] * turned[q2p]
            rows[q2] = acc
    if dual is not None:
        rows = [b + u for b, u in zip(rows, dual)]
    high, low = split(jnp.concatenate(rows, axis=1))
    sums = None
    for r2 in range(R2):
        part = slice(r2 * D, (r2 + 1) * D)
        term = dot(hot_t[r2], high[part]) + dot(hot_t[r2], low[part])
        sums = term if sums is None else sums + term
    _, rps = slice_parity(geo, (S, LANES))
    fresh = []
    for q2 in range(Q2):
        cols = slice(q2 * LANES, (q2 + 1) * LANES)
        mine = sums[0:S, cols]
        for p in range(1, RP):
            mine = jnp.where(rps == p, sums[p * S : (p + 1) * S, cols], mine)
        whole = mine
        for s in range(1, RP):
            whole = whole + jnp.where(rps >= s, roll(mine, s * geo.L), 0.0)
            whole = whole + jnp.where(rps < RP - s, roll(mine, -s * geo.L), 0.0)
        fresh.append((whole + scaled[:, cols]) / den[...])
    high, low = split(jnp.concatenate(fresh, axis=1))
    back = dot(hot[...], high) + dot(hot[...], low)
    _, rpn = slice_parity(geo, (n, LANES))
    new_dual, new_raise = [], []
    moved = jnp.zeros((1, LANES), f32)
    for q2 in range(Q2):
        cols = slice(q2 * LANES, (q2 + 1) * LANES)
        own = back[0:n, cols]
        for p in range(1, RP):
            own = jnp.where(rpn == p, back[p * n : (p + 1) * n, cols], own)
        u = (rows[q2] - own) * act[...]
        new_dual.append(u)
        new_raise.append(PENALTY * (own - u))
        step = u if dual is None else u - dual[q2]
        moved = moved + jnp.sum(step * step, axis=0, keepdims=True)
    shifted = jnp.zeros((1, LANES), f32)
    for q2 in range(Q2):
        gap = fresh[q2] if old is None else fresh[q2] - old[q2]
        shifted = shifted + jnp.sum(count[...] * gap * gap, axis=0, keepdims=True)
    return new_dual, new_raise, fresh, moved, shifted


def read_list(geo, ref):
    return [ref[:, q2 * LANES : (q2 + 1) * LANES] for q2 in range(geo.Q2)]


def write_list(geo, ref, values):
    for q2 in range(geo.Q2):
        ref[:, q2 * LANES : (q2 + 1) * LANES] = values[q2]


def owner_first(geo, slice_index, weight_in, aim_in, recv,
                send, coef, hot_t, hot, act, scaled, den, count, dual, old, norms,
                weight, aim, sems):
    X = geo.X
    copies = [pltpu.make_async_copy(x, y, sems.at[i])
              for i, (x, y) in enumerate(((weight_in, weight), (aim_in, aim)))]
    for copy in copies:
        copy.start()
    owner_setup(
        geo, slice_index[0], weight, aim, copies, recv, coef, hot_t, hot, act, scaled, den, count
    )
    tables = (coef, hot_t, hot, act, scaled, den, count)
    chunk = 2 * X + 2
    h = arrive(geo, recv, chunk, 0)
    u, v, z, p0, d0 = owner_step(geo, h, None, None, None, *tables)
    depart(geo, v, send, 2 * X, 0)
    h = arrive(geo, recv, chunk, X)
    u, v, z, p1, d1 = owner_step(geo, h, v, u, z, *tables)
    depart(geo, v, send, 2 * X, X)
    write_list(geo, dual, u)
    write_list(geo, old, z)
    norms[...] = jnp.zeros_like(norms)
    for i, value in enumerate((p0, d0, p1, d1)):
        norms[i : i + 1] = value


def owner_middle(geo, first, recv, coef, hot_t, hot, act, scaled, den, count,
                 dual, old, norms, send, dual_out, old_out, norms_out):
    X = geo.X
    tables = (coef, hot_t, hot, act, scaled, den, count)
    u, v, z = read_list(geo, dual), None, read_list(geo, old)
    norms_out[...] = norms[...]
    for s in range(2):
        h = arrive(geo, recv, 2 * X, s * X)
        u, v, z, p, d = owner_step(geo, h, v if s else None, u, z, *tables)
        depart(geo, v, send, 2 * X, s * X)
        at = 2 * (first + s)
        norms_out[at : at + 1] = p
        norms_out[at + 1 : at + 2] = d
    write_list(geo, dual_out, u)
    write_list(geo, old_out, z)


def owner_last(geo, recv, coef, hot_t, hot, act, scaled, den, count,
               dual, old, norms, send, agreed):
    X, S, RP = geo.X, geo.S, geo.RP
    tables = (coef, hot_t, hot, act, scaled, den, count)
    u, v, z = read_list(geo, dual), None, read_list(geo, old)
    h = arrive(geo, recv, X, 0)
    u, v, z, p, d = owner_step(geo, h, None, u, z, *tables)
    depart(geo, [PENALTY * x for x in u], send, X + 1, 0)
    at = 2 * (ITERS - 1)
    everything = norms[...]
    rows = everything.shape[0]
    row = iota((rows, LANES), 0)
    everything = jnp.where(row == at, p, everything)
    everything = jnp.where(row == at + 1, d, everything)
    sums = jnp.sum(everything, axis=1, keepdims=True)
    line = jnp.sum(jnp.where(row == iota((rows, LANES), 1), sums, 0.0), axis=0, keepdims=True)
    send[pl.ds(X, geo.D, stride=X + 1), :] = jnp.broadcast_to(line, (geo.D, LANES))
    part = S // RP
    _, rps = slice_parity(geo, (part, LANES))
    for q2 in range(geo.Q2):
        value = z[q2][0:part]
        for i in range(1, RP):
            value = jnp.where(rps == i, z[q2][i * part : (i + 1) * part], value)
        agreed[q2 * part : (q2 + 1) * part, :] = value


def finish(geo, base, recv, agreed, duals, consensus, norms, stage):
    X, S, RP, G, L = geo.X, geo.S, geo.RP, geo.G, geo.L
    unpack(geo, recv, stage, X + 1, 0)

    def body(f, carry):
        at = base[f]
        for q in range(geo.Q):
            duals[q, pl.ds(f, 1), :] = stage[pl.ds(at + geo.off(q), 1), :]
        return carry

    lax.fori_loop(0, geo.F, body, 0)
    part = S // RP
    n = geo.Q2 * part
    for q2 in range(geo.Q2):
        sides = [agreed[j * n + q2 * part : j * n + (q2 + 1) * part, :] for j in range(G)]
        for qp in range(2):
            for rp in range(RP):
                acc = None
                for j in range(G):
                    v = roll(sides[j], (j - (qp * RP + rp)) * L)
                    acc = v if acc is None else jnp.where(group_mask((part, LANES), j, L), v, acc)
                consensus[2 * q2 + qp, rp * part : (rp + 1) * part, :] = acc
    line = jnp.sum(recv[pl.ds(X, geo.D, stride=X + 1), :], axis=0, keepdims=True)
    line = jnp.broadcast_to(jnp.sqrt(line), (8, LANES))
    side = iota((8, LANES), 0)
    lane = iota((8, LANES), 1)
    table = jnp.zeros((8, LANES), f32)
    for i in range(ITERS):
        table = jnp.where((lane == i) & (side == 0), roll(line, -i), table)
        table = jnp.where((lane == i) & (side == 1), PENALTY * roll(line, -i - 1), table)
    norms[...] = table[:2, :ITERS]


VM = pltpu.VMEM
SM = pltpu.SMEM
HB = pltpu.HBM


def call(body, args, ins, outs, scratch=(), name=None):
    args = [
        pltpu.with_memory_space_constraint(x, HB) if s is HB else x for x, s in zip(args, ins)
    ]
    return pl.pallas_call(
        body,
        in_specs=[pl.BlockSpec(memory_space=s) for s in ins],
        out_specs=[pl.BlockSpec(memory_space=s) for _, _, s in outs],
        out_shape=[
            jax.ShapeDtypeStruct(shape, dtype) if s is VM else s(shape, dtype)
            for shape, dtype, s in outs
        ],
        scratch_shapes=list(scratch),
        compiler_params=pltpu.CompilerParams(vmem_limit_bytes=40 << 20),
        name=name,
    )(*args)


def feeder_calls(
    geo, iface, substation_of, live_count, slice_index, inverse, cost, lower, upper
):
    F, K, C, D, X = geo.F, geo.K, geo.C, geo.D, geo.X
    pieces = F // PIECE
    stage = pltpu.VMEM((geo.stage_rows, LANES), f32)
    works = (pltpu.VMEM((K, LANES), f32),) * (4 * GROUP)
    squares = pltpu.VMEM((F, K, K), bf16)
    prices = pltpu.VMEM((F, K, C), f32)
    halves = pltpu.VMEM((F, K, C), bf16)
    carried = (((F, K, C), bf16, HB), ((F, 8, C), f32, VM))

    def sems(count):
        return pltpu.SemaphoreType.DMA((count, pieces))

    def begin():
        rounded, kept, lim, base, table, send = call(
            functools.partial(feeder_first, geo),
            (iface, substation_of, live_count, slice_index, inverse, cost, lower, upper),
            (HB, HB, SM, SM, HB, HB, HB, HB),
            carried
            + (
                ((K, LANES), f32, VM),
                ((F,), i32, SM),
                (iface.shape, i32, SM),
                ((D * (2 * X + 2), LANES), f32, VM),
            ),
            (squares, prices, halves, sems(2), sems(1),
             stage, stage, pltpu.VMEM((2 * geo.NB, LANES), f32), pltpu.SMEM((geo.NB,), i32),
             pltpu.SMEM((F,), i32), pltpu.SMEM((F,), i32), pltpu.VMEM((LANES, K), f32),
             pltpu.SemaphoreType.DMA((4,)), pltpu.VMEM((K, LANES), f32)) + works,
            "feeder_first",
        )
        return (rounded, kept, lim, base, table), base, send

    def advance(state, recv, last):
        rounded, kept, lim, base, table = state
        out = call(
            functools.partial(feeder_pair, geo, last),
            (table, base, live_count, inverse, cost, rounded, kept, lim, recv),
            (SM, SM, SM, HB, HB, HB, VM, VM, VM),
            ((((F, K, C), f32, HB),) if last else carried)
            + (((D * (1 if last else 2) * X, LANES), f32, VM),),
            (squares, prices, halves, prices if last else halves, sems(3), sems(1))
            + (stage,) * (3 if last else 4) + (pltpu.VMEM((K, LANES), f32),) + works + works[: 2 * GROUP],
            "feeder_last" if last else "feeder_pair",
        )
        return out if last else ((out[0], out[1], lim, base, table), out[2])

    return begin, advance


def shards(
    n_sub,
    n_fdr,
    inverse,
    cost,
    lower_limit,
    upper_limit,
    iface_rows,
    substation_of,
    live_count,
    reserve_weight,
    reserve_target,
):
    slots, rows, scen = cost.shape
    geo = Geometry(slots, rows, iface_rows.shape[1], scen, reserve_weight.shape[0], n_sub, n_fdr)
    F, K, Q, C, S, D, X = geo.F, geo.K, geo.Q, geo.C, geo.S, geo.D, geo.X
    R2, RP, Q2 = geo.R2, geo.RP, geo.Q2
    n, wide = R2 * D, Q2 * LANES

    def swap(x):
        y = x.reshape(D, 1, x.shape[0] // D * LANES)
        y = lax.all_to_all(y, ("sub", "fdr"), split_axis=0, concat_axis=0, tiled=True)
        return y.reshape(x.shape)

    slice_index = lax.axis_index("fdr").astype(i32).reshape(1)
    begin, advance = feeder_calls(
        geo, iface_rows.T, substation_of, live_count, slice_index,
        inverse, cost, lower_limit, upper_limit,
    )
    feeders, base, send = begin()
    state = (
        ((n, wide), f32, VM),
        ((S, wide), f32, VM),
        ((16, LANES), f32, VM),
    )
    out = call(
        functools.partial(owner_first, geo),
        (slice_index, reserve_weight, jnp.swapaxes(reserve_target, 0, 1), swap(send)),
        (SM, HB, HB, VM),
        (
            ((D * 2 * X, LANES), f32, VM),
            ((2 * Q2 * Q2, n, LANES), f32, VM),
            ((R2, RP * S, D), bf16, VM),
            ((RP * n, S), bf16, VM),
            ((n, LANES), f32, VM),
            ((S, wide), f32, VM),
            ((S, LANES), f32, VM),
            ((S, LANES), f32, VM),
        )
        + state,
        (pltpu.SMEM((S,), f32), pltpu.VMEM((Q, S, C), f32), pltpu.SemaphoreType.DMA((2,))),
        "owner_first",
    )
    send, tables, memory = out[0], out[1:8], out[8:]

    for first in range(2, ITERS - 1, 2):
        feeders, send = advance(feeders, swap(send), False)
        out = call(
            functools.partial(owner_middle, geo, first),
            (swap(send), *tables, *memory),
            (VM,) * 11,
            (((D * 2 * X, LANES), f32, VM),) + state,
            (),
            "owner_middle",
        )
        send, memory = out[0], out[1:]
    setpoints, send = advance(feeders, swap(send), True)
    send, agreed = call(
        functools.partial(owner_last, geo),
        (swap(send), *tables, *memory),
        (VM,) * 11,
        (((D * (X + 1), LANES), f32, VM), ((Q2 * S // RP, LANES), f32, VM)),
        (),
        "owner_last",
    )
    gathered = lax.all_gather(agreed, "fdr", axis=0, tiled=True)
    duals, consensus, norms = call(
        functools.partial(finish, geo),
        (base, swap(send), gathered),
        (SM, VM, VM),
        (((Q, F, C), f32, VM), ((Q, S, C), f32, VM), ((2, ITERS), f32, VM)),
        (pltpu.VMEM((geo.stage_rows, LANES), f32),),
        "finish",
    )
    return jnp.swapaxes(duals, 0, 1), jnp.swapaxes(consensus, 0, 1), norms.T, setpoints


def solution(mesh):
    placed = (
        P(("sub", "fdr"), None, None),
        P(("sub", "fdr"), None, None),
        P(("sub", "fdr"), None),
        P(("sub", "fdr"), None),
        P(("sub", "fdr"), None),
        P(("sub", "fdr")),
        P(("sub", "fdr")),
        P("sub"),
        P("sub", None, None),
    )
    return jax.shard_map(
        functools.partial(shards, mesh.shape["sub"], mesh.shape["fdr"]),
        mesh=mesh,
        in_specs=placed,
        out_specs=(
            P(("sub", "fdr"), None, None),
            P("sub", None, None),
            P(),
            P(("sub", "fdr"), None, None),
        ),
        check_vma=False,
    )
```

```python
import functools

import jax
import jax.numpy as jnp
from jax import lax
from jax.experimental import pallas as pl
from jax.experimental.pallas import tpu as pltpu
from jax.sharding import PartitionSpec as P

ITERS = 5
PENALTY = 2.0
LANES = 128
THIN = 16
GROUP = 8
PIECE = 8

f32 = jnp.float32
bf16 = jnp.bfloat16
i32 = jnp.int32


class Geometry:
    def __init__(self, slots, rows, ifc, scen, owned, n_sub, n_fdr):
        self.F, self.K, self.Q, self.C, self.S = slots, rows, ifc, scen, owned
        self.NB, self.G = n_sub, n_fdr
        self.D = n_sub * n_fdr
        overflow = max(1, slots // (2 * n_sub))
        cap = max(2, slots // n_sub + overflow)
        self.L = scen // n_fdr
        self.RP = n_fdr // 2
        self.R2 = -(-cap // self.RP)
        self.PR = self.R2 * self.RP
        self.Q2 = ifc // 2
        self.X = self.Q2 * self.R2
        self.stage_rows = self.G * self.X * self.NB
        self.id_lane = self.Q2 * self.PR * self.Q

    def off(self, q):
        q2, qp = divmod(q, 2)
        return (qp * self.RP * self.X + q2 * self.R2) * self.NB


def iota(shape, dim):
    return lax.broadcasted_iota(i32, shape, dim)


def group_mask(shape, g, width):
    lane = iota(shape, 1)
    return (lane >= g * width) & (lane < (g + 1) * width)


def roll(x, shift):
    shift = shift % LANES
    return pltpu.roll(x, shift, 1) if shift else x


def pack(geo, stage, send, chunk, off):
    n = geo.X * geo.NB
    for j in range(geo.G):
        acc = None
        for g in range(geo.G):
            v = roll(stage[g * n : (g + 1) * n, :], (g - j) * geo.L)
            acc = v if acc is None else jnp.where(group_mask((n, LANES), g, geo.L), v, acc)
        for x in range(geo.X):
            send[pl.ds(j * chunk + off + x, geo.NB, stride=geo.G * chunk), :] = acc[
                x * geo.NB : (x + 1) * geo.NB
            ]


def unpack(geo, recv, stage, chunk, off):
    n = geo.X * geo.NB
    parts = [
        jnp.concatenate(
            [
                recv[pl.ds(j * chunk + off + x, geo.NB, stride=geo.G * chunk), :]
                for x in range(geo.X)
            ],
            axis=0,
        )
        for j in range(geo.G)
    ]
    for g in range(geo.G):
        acc = None
        for j in range(geo.G):
            v = roll(parts[j], (j - g) * geo.L)
            acc = v if acc is None else jnp.where(group_mask((n, LANES), j, geo.L), v, acc)
        stage[g * n : (g + 1) * n, :] = acc


def dot(a, b):
    return jnp.dot(a, b, preferred_element_type=f32)


def limits(geo, turned, u):
    shape = (geo.K, LANES)
    low = jnp.broadcast_to(turned[:, u : u + 1], shape)
    return low, jnp.broadcast_to(turned[:, geo.F + u : geo.F + u + 1], shape)


def clip(x, low, high):
    return jnp.minimum(jnp.maximum(x, low), high)


def moves(pairs, sems, size):
    def one(i, c):
        src, dst = pairs[i]
        part = pl.ds(c * size, size)
        return pltpu.make_async_copy(src.at[part], dst.at[part], sems.at[i, c])

    return min(pairs[0][0].shape[0], pairs[0][1].shape[0]) // size, one


def sweep(slots, body):
    for near in (False, True):

        def step(i, carry, near=near):
            body(i * GROUP, GROUP, near)
            return carry

        half = slots // 2 // GROUP
        lax.fori_loop(half if near else 0, 2 * half if near else half, step, 0)


def pick(work, iface, f, q):
    return work[pl.ds(iface[q, f], 1), :]


def put(f, t, near, out, nearby):
    if near:
        nearby[f - nearby.shape[0]] = t
    else:
        out[f] = t


def feeder_first(geo, rows_in, sub_in, live, slice_index, inverse, cost, lower, upper,
                 far, nearby, kept, lim, base, iface, send,
                 inv, price, out, sems, out_sems,
                 stage1, stage2, meta, count, rank, sub, edge, edge_sems, turned, *works):
    F, K, Q, NB, X = geo.F, geo.K, geo.Q, geo.NB, geo.X
    chunk = 2 * X + 2
    bound, square, left, ahead = (works[i * GROUP : (i + 1) * GROUP] for i in range(4))
    pieces, load = moves(((inverse, inv), (cost, price)), sems, PIECE)
    far_pieces, store = moves(((out, far),), out_sems, PIECE)
    sides = [
        pltpu.make_async_copy(x, edge.at[pl.ds(i * F, F)], edge_sems.at[i])
        for i, x in enumerate((lower, upper))
    ]
    tables = [
        pltpu.make_async_copy(x, y, edge_sems.at[2 + i])
        for i, (x, y) in enumerate(((sub_in, sub), (rows_in, iface)))
    ]
    for copy in tables + sides:
        copy.start()
    for c in range(pieces):
        for i in range(2):
            load(i, c).start()
    for copy in tables:
        copy.wait()
    for k in range(NB):
        count[k] = 0

    def place(f, carry):
        k = lax.div(sub[f], geo.S)
        r = count[k]
        count[k] = r + 1
        rank[f] = r
        base[f] = (lax.rem(r, geo.RP) * X + lax.div(r, geo.RP)) * NB + k
        return carry

    lax.fori_loop(0, F, place, 0)
    edge[2 * F :, :] = jnp.zeros((LANES - 2 * F, K), f32)
    for copy in sides:
        copy.wait()
    lim[...] = edge[...].T
    stage1[...] = jnp.zeros_like(stage1)
    stage2[...] = jnp.zeros_like(stage2)
    meta[...] = jnp.zeros_like(meta)
    kept[...] = jnp.zeros_like(kept)
    lane = iota((1, LANES), 1)
    third = jnp.zeros((1, LANES), i32)
    for i in range(1, geo.Q2 + 1):
        third = third + jnp.where(lane >= i * geo.PR * Q, 1, 0)
    within = lane - third * (geo.PR * Q)

    def body(at, size, near):
        for c in range(size // PIECE):
            for i in range(2):
                load(i, at // PIECE + c).wait()
        fs = [at + u for u in range(size)]
        turned[...] = pltpu.roll(lim[...], LANES - at, 1)
        for u, f in enumerate(fs):
            place_of = within - rank[f] * Q
            chosen = jnp.full((1, LANES), -1, i32)
            for q in range(Q):
                chosen = jnp.where((place_of == q) & (third < geo.Q2), iface[q, f], chosen)
            hot = (iota((K, LANES), 0) == jnp.broadcast_to(chosen, (K, LANES))).astype(f32)
            price_u = price[f]
            both = dot(inv[f], jnp.concatenate([-price_u, hot], axis=1).astype(bf16))
            primal = both[:, :LANES]
            bound[u][...] = primal
            square[u][...] = both[:, LANES:]
            low, high = limits(geo, turned, u)
            t = clip(primal, low, high) - price_u
            left[u][...] = t
            t = t.astype(bf16)
            put(f, t, near, out, nearby)
            ahead[u][...] = dot(inv[f], t)
            if not near and u % PIECE == PIECE - 1:
                store(0, at // PIECE + u // PIECE).start()
        for u, f in enumerate(fs):
            k = lax.div(sub[f], geo.S)
            ident = jnp.where(f < live[0], sub[f] - k * geo.S + 1, 0).astype(f32)
            lines = [jnp.where(lane == geo.id_lane + rank[f], ident, 0.0),
                     jnp.zeros((1, LANES), f32)]
            to = base[f]
            for q in range(Q):
                m, i = divmod(q, geo.Q2)
                lines[m] = lines[m] + jnp.where(third == i, pick(square[u], iface, f, q), 0.0)
                stage1[pl.ds(to + geo.off(q), 1), :] = pick(bound[u], iface, f, q)
                stage2[pl.ds(to + geo.off(q), 1), :] = pick(ahead[u], iface, f, q)
                kept[f, q : q + 1, :] = pick(left[u], iface, f, q)
            for m in range(2):
                spot = pl.ds(m * NB + k, 1)
                meta[spot, :] = meta[spot, :] + lines[m]

    sweep(F, body)
    pack(geo, stage1, send, chunk, 0)
    pack(geo, stage2, send, chunk, X)
    for j in range(geo.G):
        for m in range(2):
            send[pl.ds(j * chunk + 2 * X + m, NB, stride=geo.G * chunk), :] = meta[
                m * NB : (m + 1) * NB
            ]
    for c in range(far_pieces):
        store(0, c).wait()


def raise_rows(geo, f, iface, base, rows, work, stage):
    at = base[f]
    rows = [rows[q] + stage[pl.ds(at + geo.off(q), 1), :] for q in range(geo.Q)]
    for q in range(geo.Q):
        work[pl.ds(iface[q, f], 1), :] = rows[q]


def feeder_pair(geo, last, iface, base, live, inverse, cost, far, nearby, kept, lim, recv, *rest):
    if last:
        result, send, inv, price, held, out, sems, out_sems = rest[:8]
        rest = rest[8:]
    else:
        result, nearby_out, kept_out, send, inv, price, held, out, sems, out_sems = rest[:10]
        rest = rest[10:]
    ways = 1 if last else 2
    arrived, leaving, works = rest[:2], rest[2 : 2 + ways], rest[2 + ways :]
    turned, works = works[0], works[1:]
    side, bound, left, ahead, lows, highs = (works[i * GROUP : (i + 1) * GROUP] for i in range(6))
    pieces, load = moves(((inverse, inv), (cost, price), (far, held)), sems, PIECE)
    out_pieces, store = moves(((out, result),), out_sems, PIECE)
    for c in range(pieces):
        for i in range(3 if 2 * c < pieces else 2):
            load(i, c).start()
    for s in range(2):
        unpack(geo, recv, arrived[s], 2 * geo.X, s * geo.X)
    for stage in leaving:
        stage[...] = jnp.zeros_like(stage)
    if not last:
        kept_out[...] = jnp.zeros_like(kept_out)

    def body(at, size, near):
        for c in range(size // PIECE):
            for i in range(2 if near else 3):
                load(i, at // PIECE + c).wait()
        fs = [at + u for u in range(size)]
        turned[...] = pltpu.roll(lim[...], LANES - at, 1)
        for u, f in enumerate(fs):
            side[u][...] = (nearby[f - nearby.shape[0]] if near else held[f]).astype(f32)
            rows = [kept[f, q : q + 1, :] for q in range(geo.Q)]
            raise_rows(geo, f, iface, base, rows, side[u], arrived[0])
        for u, f in enumerate(fs):
            low, high = limits(geo, turned, u)
            lows[u][...] = low
            highs[u][...] = high
            left[u][...] = clip(dot(inv[f], side[u][...].astype(bf16)), low, high) - price[f]
        for u, f in enumerate(fs):
            rows = [pick(left[u], iface, f, q) for q in range(geo.Q)]
            raise_rows(geo, f, iface, base, rows, left[u], arrived[1])
        for u, f in enumerate(fs):
            low, high = lows[u][...], highs[u][...]
            primal = dot(inv[f], left[u][...].astype(bf16))
            bound[u][...] = primal
            anchor = clip(primal, low, high)
            if last:
                out[f] = anchor * jnp.where(f < live[0], 1.0, 0.0)
            else:
                t = anchor - price[f]
                side[u][...] = t
                t = t.astype(bf16)
                put(f, t, near, out, nearby_out)
                ahead[u][...] = dot(inv[f], t)
            if (last or not near) and u % PIECE == PIECE - 1:
                store(0, at // PIECE + u // PIECE).start()
        for u, f in enumerate(fs):
            to = base[f]
            for q in range(geo.Q):
                leaving[0][pl.ds(to + geo.off(q), 1), :] = pick(bound[u], iface, f, q)
                if not last:
                    leaving[1][pl.ds(to + geo.off(q), 1), :] = pick(ahead[u], iface, f, q)
                    kept_out[f, q : q + 1, :] = pick(side[u], iface, f, q)

    sweep(geo.F, body)
    for s in range(ways):
        pack(geo, leaving[s], send, ways * geo.X, s * geo.X)
    for c in range(out_pieces):
        store(0, c).wait()


def slice_parity(geo, shape):
    lane = iota(shape, 1)
    half = geo.RP * geo.L
    qp = jnp.where(lane >= half, 1, 0)
    inner = lane - qp * half
    rp = jnp.zeros(shape, i32)
    for i in range(1, geo.RP):
        rp = rp + jnp.where(inner >= i * geo.L, 1, 0)
    return qp, rp


def owner_setup(
    geo, slice_index, weight, aim, copies, recv, coef, hot_t, hot, act, scaled, den, count
):
    X, D, S, Q, Q2, R2, RP, PR = geo.X, geo.D, geo.S, geo.Q, geo.Q2, geo.R2, geo.RP, geo.PR
    chunk = 2 * X + 2
    metas = [recv[pl.ds(2 * X + m, D, stride=chunk), :] for m in range(2)]
    qp, rp = slice_parity(geo, (D, LANES))
    padded = metas[0]
    if D < LANES:
        padded = jnp.concatenate([padded, jnp.zeros((LANES - D, LANES), f32)], axis=0)
    turned = padded.T
    total = jnp.zeros((S, D), f32)
    for r2 in range(R2):
        live = jnp.zeros((D, LANES), f32)
        for p in range(RP):
            r = r2 * RP + p
            col = metas[0][:, geo.id_lane + r : geo.id_lane + r + 1]
            wide = jnp.broadcast_to(col, (D, LANES))
            live = jnp.where(rp == p, jnp.where(wide > 0.5, 1.0, 0.0), live)
            mine = (wide == (iota((D, LANES), 1) + 1).astype(f32)).astype(f32)
            hot[(p * R2 + r2) * D : (p * R2 + r2 + 1) * D, :] = mine[:, :S].astype(bf16)
            row = turned[geo.id_lane + r : geo.id_lane + r + 1, :D]
            theirs = (
                jnp.broadcast_to(row, (S, D)) == (iota((S, D), 0) + 1).astype(f32)
            ).astype(f32)
            total = total + theirs
            hot_t[r2, p * S : (p + 1) * S, :] = theirs.astype(bf16)
        act[r2 * D : (r2 + 1) * D, :] = live
    for par in range(2):
        for q2 in range(Q2):
            for q2p in range(Q2):
                for r2 in range(R2):
                    sides = []
                    for side in range(2):
                        q = 2 * q2 + side
                        other = 2 * q2p + (side if par == 0 else 1 - side)
                        sides.append((q // Q2, (q % Q2) * PR * Q + r2 * RP * Q + other))
                    idx = rp * Q + jnp.where(qp == 0, sides[0][1], sides[1][1])
                    if sides[0][0] == sides[1][0]:
                        value = jnp.take_along_axis(metas[sides[0][0]], idx, axis=1)
                    else:
                        value = jnp.where(
                            qp == 0,
                            jnp.take_along_axis(metas[sides[0][0]], idx, axis=1),
                            jnp.take_along_axis(metas[sides[1][0]], idx, axis=1),
                        )
                    coef[(par * Q2 + q2) * Q2 + q2p, r2 * D : (r2 + 1) * D, :] = value
    for copy in copies:
        copy.wait()
    members = jnp.sum(total, axis=1, keepdims=True)
    w = jnp.zeros((S, LANES), f32)
    for s in range(S):
        w = jnp.where(iota((S, LANES), 0) == s, weight[s], w)
    members = jnp.broadcast_to(members, (S, LANES))
    den[...] = members + w
    qps, rps = slice_parity(geo, (S, LANES))
    count[...] = jnp.where(rps == 0, members, 0.0)
    lane = iota((S, LANES), 1)
    inner = lane - (qps * RP + rps) * geo.L
    index = inner + slice_index * geo.L
    for q2 in range(Q2):
        even = jnp.take_along_axis(aim[2 * q2], index, axis=1)
        odd = jnp.take_along_axis(aim[2 * q2 + 1], index, axis=1)
        scaled[:, q2 * LANES : (q2 + 1) * LANES] = w * jnp.where(qps == 0, even, odd)


def arrive(geo, recv, chunk, off):
    return [
        jnp.concatenate(
            [
                recv[pl.ds(off + q2 * geo.R2 + r2, geo.D, stride=chunk), :]
                for r2 in range(geo.R2)
            ],
            axis=0,
        )
        for q2 in range(geo.Q2)
    ]


def depart(geo, values, send, chunk, off):
    for q2 in range(geo.Q2):
        for r2 in range(geo.R2):
            send[pl.ds(off + q2 * geo.R2 + r2, geo.D, stride=chunk), :] = values[q2][
                r2 * geo.D : (r2 + 1) * geo.D
            ]


def split(x):
    high = x.astype(bf16)
    return high, (x - high.astype(f32)).astype(bf16)


def owner_step(geo, h, raised, dual, old, coef, hot_t, hot, act, scaled, den, count):
    D, S, Q2, R2, RP = geo.D, geo.S, geo.Q2, geo.R2, geo.RP
    n = R2 * D
    rows = list(h)
    if raised is not None:
        turned = [roll(v, geo.RP * geo.L) for v in raised]
        for q2 in range(Q2):
            acc = rows[q2]
            for q2p in range(Q2):
                acc = acc + coef[q2 * Q2 + q2p] * raised[q2p]
                acc = acc + coef[(Q2 + q2) * Q2 + q2p] * turned[q2p]
            rows[q2] = acc
    if dual is not None:
        rows = [b + u for b, u in zip(rows, dual)]
    high, low = split(jnp.concatenate(rows, axis=1))
    sums = None
    for r2 in range(R2):
        part = slice(r2 * D, (r2 + 1) * D)
        term = dot(hot_t[r2], high[part]) + dot(hot_t[r2], low[part])
        sums = term if sums is None else sums + term
    _, rps = slice_parity(geo, (S, LANES))
    fresh = []
    for q2 in range(Q2):
        cols = slice(q2 * LANES, (q2 + 1) * LANES)
        mine = sums[0:S, cols]
        for p in range(1, RP):
            mine = jnp.where(rps == p, sums[p * S : (p + 1) * S, cols], mine)
        whole = mine
        for s in range(1, RP):
            whole = whole + jnp.where(rps >= s, roll(mine, s * geo.L), 0.0)
            whole = whole + jnp.where(rps < RP - s, roll(mine, -s * geo.L), 0.0)
        fresh.append((whole + scaled[:, cols]) / den[...])
    high, low = split(jnp.concatenate(fresh, axis=1))
    back = dot(hot[...], high) + dot(hot[...], low)
    _, rpn = slice_parity(geo, (n, LANES))
    new_dual, new_raise = [], []
    moved = jnp.zeros((1, LANES), f32)
    for q2 in range(Q2):
        cols = slice(q2 * LANES, (q2 + 1) * LANES)
        own = back[0:n, cols]
        for p in range(1, RP):
            own = jnp.where(rpn == p, back[p * n : (p + 1) * n, cols], own)
        u = (rows[q2] - own) * act[...]
        new_dual.append(u)
        new_raise.append(PENALTY * (own - u))
        step = u if dual is None else u - dual[q2]
        moved = moved + jnp.sum(step * step, axis=0, keepdims=True)
    shifted = jnp.zeros((1, LANES), f32)
    for q2 in range(Q2):
        gap = fresh[q2] if old is None else fresh[q2] - old[q2]
        shifted = shifted + jnp.sum(count[...] * gap * gap, axis=0, keepdims=True)
    return new_dual, new_raise, fresh, moved, shifted


def read_list(geo, ref):
    return [ref[:, q2 * LANES : (q2 + 1) * LANES] for q2 in range(geo.Q2)]


def write_list(geo, ref, values):
    for q2 in range(geo.Q2):
        ref[:, q2 * LANES : (q2 + 1) * LANES] = values[q2]


def owner_first(geo, slice_index, weight_in, aim_in, recv,
                send, coef, hot_t, hot, act, scaled, den, count, dual, old, norms,
                weight, aim, sems):
    X = geo.X
    copies = [pltpu.make_async_copy(x, y, sems.at[i])
              for i, (x, y) in enumerate(((weight_in, weight), (aim_in, aim)))]
    for copy in copies:
        copy.start()
    owner_setup(
        geo, slice_index[0], weight, aim, copies, recv, coef, hot_t, hot, act, scaled, den, count
    )
    tables = (coef, hot_t, hot, act, scaled, den, count)
    chunk = 2 * X + 2
    h = arrive(geo, recv, chunk, 0)
    u, v, z, p0, d0 = owner_step(geo, h, None, None, None, *tables)
    depart(geo, v, send, 2 * X, 0)
    h = arrive(geo, recv, chunk, X)
    u, v, z, p1, d1 = owner_step(geo, h, v, u, z, *tables)
    depart(geo, v, send, 2 * X, X)
    write_list(geo, dual, u)
    write_list(geo, old, z)
    norms[...] = jnp.zeros_like(norms)
    for i, value in enumerate((p0, d0, p1, d1)):
        norms[i : i + 1] = value


def owner_middle(geo, first, recv, coef, hot_t, hot, act, scaled, den, count,
                 dual, old, norms, send, dual_out, old_out, norms_out):
    X = geo.X
    tables = (coef, hot_t, hot, act, scaled, den, count)
    u, v, z = read_list(geo, dual), None, read_list(geo, old)
    norms_out[...] = norms[...]
    for s in range(2):
        h = arrive(geo, recv, 2 * X, s * X)
        u, v, z, p, d = owner_step(geo, h, v if s else None, u, z, *tables)
        depart(geo, v, send, 2 * X, s * X)
        at = 2 * (first + s)
        norms_out[at : at + 1] = p
        norms_out[at + 1 : at + 2] = d
    write_list(geo, dual_out, u)
    write_list(geo, old_out, z)


def owner_last(geo, recv, coef, hot_t, hot, act, scaled, den, count,
               dual, old, norms, send, agreed):
    X, S, RP = geo.X, geo.S, geo.RP
    tables = (coef, hot_t, hot, act, scaled, den, count)
    u, v, z = read_list(geo, dual), None, read_list(geo, old)
    h = arrive(geo, recv, X, 0)
    u, v, z, p, d = owner_step(geo, h, None, u, z, *tables)
    depart(geo, [PENALTY * x for x in u], send, X + 1, 0)
    at = 2 * (ITERS - 1)
    everything = norms[...]
    rows = everything.shape[0]
    row = iota((rows, LANES), 0)
    everything = jnp.where(row == at, p, everything)
    everything = jnp.where(row == at + 1, d, everything)
    sums = jnp.sum(everything, axis=1, keepdims=True)
    line = jnp.sum(jnp.where(row == iota((rows, LANES), 1), sums, 0.0), axis=0, keepdims=True)
    send[pl.ds(X, geo.D, stride=X + 1), :] = jnp.broadcast_to(line, (geo.D, LANES))
    part = S // RP
    _, rps = slice_parity(geo, (part, LANES))
    for q2 in range(geo.Q2):
        value = z[q2][0:part]
        for i in range(1, RP):
            value = jnp.where(rps == i, z[q2][i * part : (i + 1) * part], value)
        agreed[q2 * part : (q2 + 1) * part, :] = value


def finish(geo, base, recv, agreed, duals, consensus, norms, stage):
    X, S, RP, G, L = geo.X, geo.S, geo.RP, geo.G, geo.L
    unpack(geo, recv, stage, X + 1, 0)

    def body(f, carry):
        at = base[f]
        for q in range(geo.Q):
            duals[q, pl.ds(f, 1), :] = stage[pl.ds(at + geo.off(q), 1), :]
        return carry

    lax.fori_loop(0, geo.F, body, 0)
    part = S // RP
    n = geo.Q2 * part
    for q2 in range(geo.Q2):
        sides = [agreed[j * n + q2 * part : j * n + (q2 + 1) * part, :] for j in range(G)]
        for qp in range(2):
            for rp in range(RP):
                acc = None
                for j in range(G):
                    v = roll(sides[j], (j - (qp * RP + rp)) * L)
                    acc = v if acc is None else jnp.where(group_mask((part, LANES), j, L), v, acc)
                consensus[2 * q2 + qp, rp * part : (rp + 1) * part, :] = acc
    line = jnp.sum(recv[pl.ds(X, geo.D, stride=X + 1), :], axis=0, keepdims=True)
    line = jnp.broadcast_to(jnp.sqrt(line), (8, LANES))
    side = iota((8, LANES), 0)
    lane = iota((8, LANES), 1)
    table = jnp.zeros((8, LANES), f32)
    for i in range(ITERS):
        table = jnp.where((lane == i) & (side == 0), roll(line, -i), table)
        table = jnp.where((lane == i) & (side == 1), PENALTY * roll(line, -i - 1), table)
    norms[...] = table[:2, :ITERS]


VM = pltpu.VMEM
SM = pltpu.SMEM
HB = pltpu.HBM


def call(body, args, ins, outs, scratch=(), name=None):
    args = [
        pltpu.with_memory_space_constraint(x, HB) if s is HB else x for x, s in zip(args, ins)
    ]
    return pl.pallas_call(
        body,
        in_specs=[pl.BlockSpec(memory_space=s) for s in ins],
        out_specs=[pl.BlockSpec(memory_space=s) for _, _, s in outs],
        out_shape=[
            jax.ShapeDtypeStruct(shape, dtype) if s is VM else s(shape, dtype)
            for shape, dtype, s in outs
        ],
        scratch_shapes=list(scratch),
        compiler_params=pltpu.CompilerParams(vmem_limit_bytes=40 << 20),
        name=name,
    )(*args)


def feeder_calls(
    geo, iface, substation_of, live_count, slice_index, inverse, cost, lower, upper
):
    F, K, C, D, X = geo.F, geo.K, geo.C, geo.D, geo.X
    pieces = F // PIECE
    stage = pltpu.VMEM((geo.stage_rows, LANES), f32)
    works = (pltpu.VMEM((K, LANES), f32),) * (4 * GROUP)
    squares = pltpu.VMEM((F, K, K), bf16)
    prices = pltpu.VMEM((F, K, C), f32)
    halves = pltpu.VMEM((F // 2, K, C), bf16)
    half = (F // 2, K, C)
    carried = ((half, bf16, HB), (half, bf16, VM), ((F, 8, C), f32, VM))

    def sems(count):
        return pltpu.SemaphoreType.DMA((count, pieces))

    def begin():
        far, nearby, kept, lim, base, table, send = call(
            functools.partial(feeder_first, geo),
            (iface, substation_of, live_count, slice_index, inverse, cost, lower, upper),
            (HB, HB, SM, SM, HB, HB, HB, HB),
            carried
            + (
                ((K, LANES), f32, VM),
                ((F,), i32, SM),
                (iface.shape, i32, SM),
                ((D * (2 * X + 2), LANES), f32, VM),
            ),
            (squares, prices, halves, sems(2), sems(1),
             stage, stage, pltpu.VMEM((2 * geo.NB, LANES), f32), pltpu.SMEM((geo.NB,), i32),
             pltpu.SMEM((F,), i32), pltpu.SMEM((F,), i32), pltpu.VMEM((LANES, K), f32),
             pltpu.SemaphoreType.DMA((4,)), pltpu.VMEM((K, LANES), f32)) + works,
            "feeder_first",
        )
        return (far, nearby, kept, lim, base, table), base, send

    def advance(state, recv, last):
        far, nearby, kept, lim, base, table = state
        out = call(
            functools.partial(feeder_pair, geo, last),
            (table, base, live_count, inverse, cost, far, nearby, kept, lim, recv),
            (SM, SM, SM, HB, HB, HB, VM, VM, VM, VM),
            ((((F, K, C), f32, HB),) if last else carried)
            + (((D * (1 if last else 2) * X, LANES), f32, VM),),
            (squares, prices, halves, prices if last else halves, sems(3), sems(1))
            + (stage,) * (3 if last else 4) + (pltpu.VMEM((K, LANES), f32),) + works + works[: 2 * GROUP],
            "feeder_last" if last else "feeder_pair",
        )
        return out if last else ((*out[:3], lim, base, table), out[3])

    return begin, advance


def shards(
    n_sub,
    n_fdr,
    inverse,
    cost,
    lower_limit,
    upper_limit,
    iface_rows,
    substation_of,
    live_count,
    reserve_weight,
    reserve_target,
):
    slots, rows, scen = cost.shape
    geo = Geometry(slots, rows, iface_rows.shape[1], scen, reserve_weight.shape[0], n_sub, n_fdr)
    F, K, Q, C, S, D, X = geo.F, geo.K, geo.Q, geo.C, geo.S, geo.D, geo.X
    R2, RP, Q2 = geo.R2, geo.RP, geo.Q2
    n, wide = R2 * D, Q2 * LANES

    def swap(x):
        y = x.reshape(D, 1, x.shape[0] // D * LANES)
        y = lax.all_to_all(y, ("sub", "fdr"), split_axis=0, concat_axis=0, tiled=True)
        return y.reshape(x.shape)

    slice_index = lax.axis_index("fdr").astype(i32).reshape(1)
    begin, advance = feeder_calls(
        geo, iface_rows.T, substation_of, live_count, slice_index,
        inverse, cost, lower_limit, upper_limit,
    )
    feeders, base, send = begin()
    state = (
        ((n, wide), f32, VM),
        ((S, wide), f32, VM),
        ((16, LANES), f32, VM),
    )
    out = call(
        functools.partial(owner_first, geo),
        (slice_index, reserve_weight, jnp.swapaxes(reserve_target, 0, 1), swap(send)),
        (SM, HB, HB, VM),
        (
            ((D * 2 * X, LANES), f32, VM),
            ((2 * Q2 * Q2, n, LANES), f32, VM),
            ((R2, RP * S, D), bf16, VM),
            ((RP * n, S), bf16, VM),
            ((n, LANES), f32, VM),
            ((S, wide), f32, VM),
            ((S, LANES), f32, VM),
            ((S, LANES), f32, VM),
        )
        + state,
        (pltpu.SMEM((S,), f32), pltpu.VMEM((Q, S, C), f32), pltpu.SemaphoreType.DMA((2,))),
        "owner_first",
    )
    send, tables, memory = out[0], out[1:8], out[8:]

    for first in range(2, ITERS - 1, 2):
        feeders, send = advance(feeders, swap(send), False)
        out = call(
            functools.partial(owner_middle, geo, first),
            (swap(send), *tables, *memory),
            (VM,) * 11,
            (((D * 2 * X, LANES), f32, VM),) + state,
            (),
            "owner_middle",
        )
        send, memory = out[0], out[1:]
    setpoints, send = advance(feeders, swap(send), True)
    send, agreed = call(
        functools.partial(owner_last, geo),
        (swap(send), *tables, *memory),
        (VM,) * 11,
        (((D * (X + 1), LANES), f32, VM), ((Q2 * S // RP, LANES), f32, VM)),
        (),
        "owner_last",
    )
    gathered = lax.all_gather(agreed, "fdr", axis=0, tiled=True)
    duals, consensus, norms = call(
        functools.partial(finish, geo),
        (base, swap(send), gathered),
        (SM, VM, VM),
        (((Q, F, C), f32, VM), ((Q, S, C), f32, VM), ((2, ITERS), f32, VM)),
        (pltpu.VMEM((geo.stage_rows, LANES), f32),),
        "finish",
    )
    return jnp.swapaxes(duals, 0, 1), jnp.swapaxes(consensus, 0, 1), norms.T, setpoints


def solution(mesh):
    placed = (
        P(("sub", "fdr"), None, None),
        P(("sub", "fdr"), None, None),
        P(("sub", "fdr"), None),
        P(("sub", "fdr"), None),
        P(("sub", "fdr"), None),
        P(("sub", "fdr")),
        P(("sub", "fdr")),
        P("sub"),
        P("sub", None, None),
    )
    return jax.shard_map(
        functools.partial(shards, mesh.shape["sub"], mesh.shape["fdr"]),
        mesh=mesh,
        in_specs=placed,
        out_specs=(
            P(("sub", "fdr"), None, None),
            P("sub", None, None),
            P(),
            P(("sub", "fdr"), None, None),
        ),
        check_vma=False,
    )
```
